128 devices in a mesh: gx: 4 (over z), gy: 4 (over y), gz: 8 (over x, core).
Axes of the slice: x: 4, y: 4, z: 4, core: 2. Of those that a mesh axis runs over, the one named last changes fastest.
Arguments:
- interact: bfloat16 [16, 32768, 512], P(None, ('gx', 'gy', 'gz')), may hold values from -6 to 6
- weight_one: bfloat16 [512, 1024], replicated, may hold values from -0.25 to 0.25
- bias_one: float32 [1024], replicated, may hold values from -3 to 3
- weight_two: bfloat16 [1024, 1024], replicated, may hold values from -0.1875 to 0.1875
- bias_two: float32 [1024], replicated, may hold values from -3 to 3
- weight_three: bfloat16 [1024, 512], replicated, may hold values from -0.1875 to 0.1875
- bias_three: float32 [512], replicated, may hold values from -3 to 3
- weight_four: bfloat16 [512, 256], replicated, may hold values from -0.25 to 0.25
- bias_four: float32 [256], replicated, may hold values from -3 to 3
- weight_out: bfloat16 [256, 1], replicated, may hold values from -1 to 1
- bias_out: float32 [1], replicated, may hold values from -1.5 to 0
- bucket_index: int32 [16, 32768], P(None, ('gx', 'gy', 'gz')), may hold values from 0 to 4095
- labels: int32 [16, 32768], P(None, ('gx', 'gy', 'gz')), may hold values from 0 to 1
Outputs:
- bucket_stats: float32 [16, 4, 4096], P(None, None, 'gx')
- summary: float32 [16, 4], replicated
The draws below stay inside these ranges and needn't reach their ends.
All inputs are finite; a program needn't handle non-finite values.
Results may differ from the reference program's by a relative error of at most 0.0045.
Values sent between devices are 32-bit elements; how exact they have to be, the bound alone decides.
No kernel may reach another device: no remote copies, remote signals or barrier semaphores. Data moves between devices by JAX's collectives and lax.ppermute only.
A program may use at most 128 MiB of HBM per device.

```python
import jax
import jax.numpy as jnp
from jax import lax

DIN = 512
H1 = 1024
H2 = 1024
H3 = 512
H4 = 256
NBUCK = 4096
STEPS = 16
EXAMPLES = 32768


def label_and_bucket(key):
    base_key = jax.random.fold_in(key, 7103)
    subkeys = jax.random.split(base_key, 3)
    positions = jnp.arange(EXAMPLES, dtype=jnp.int32)[None, :]
    threshold = 100 + 300 * positions // EXAMPLES
    dice_roll = jax.random.randint(subkeys[0], (STEPS, EXAMPLES), 0, 1000, dtype=jnp.int32)
    clicked = (dice_roll < threshold).astype(jnp.int32)
    lower_draw = jax.random.randint(subkeys[1], (STEPS, EXAMPLES), 0, NBUCK, dtype=jnp.int32)
    upper_draw = jax.random.randint(subkeys[2], (STEPS, EXAMPLES), 0, NBUCK, dtype=jnp.int32)
    buckets = jnp.where(clicked == 1, jnp.maximum(lower_draw, upper_draw), lower_draw)
    return (clicked, buckets)


def draw_labels(key, part):
    return label_and_bucket(key)[0]


def draw_bucket_index(key, part):
    return label_and_bucket(key)[1]


def level_of(own_key, extent, cuts, low, top_value):
    factor_of = 1.0
    for position, blocks in cuts:
        draws = jax.random.uniform(jax.random.fold_in(jax.random.fold_in(own_key, 6), position), (blocks,), jnp.float32, low / len(cuts), top_value / len(cuts))
        factor_of = factor_of * jnp.repeat(jnp.exp(draws), extent[position] // blocks).reshape((-1,) + (1,) * (len(extent) - 1 - position))
    return factor_of


def scatter_about(stream_key, shape, spread, bound, shards=(), kind=jnp.bfloat16):
    gain = level_of(stream_key, shape, shards, -0.22, 0.18) if shards else 1.0
    array = jax.random.normal(stream_key, shape, jnp.float32) * spread * gain
    return jnp.minimum(jnp.maximum(array, -bound), bound).astype(kind)


def setup_inputs(seed: int = 0) -> dict:
    key_list = jax.random.split(jax.random.key(seed), 14)
    return {
        "interact": scatter_about(key_list[0], (STEPS, EXAMPLES, DIN), 1.0, 6.0, ((1, 128),)),
        "weight_one": scatter_about(key_list[1], (DIN, H1), DIN ** -0.5, 0.25),
        "bias_one": scatter_about(key_list[2], (H1,), 0.5, 3.0, (), jnp.float32),
        "weight_two": scatter_about(key_list[3], (H1, H2), H1 ** -0.5, 0.1875),
        "bias_two": scatter_about(key_list[4], (H2,), 0.5, 3.0, (), jnp.float32),
        "weight_three": scatter_about(key_list[5], (H2, H3), H2 ** -0.5, 0.1875),
        "bias_three": scatter_about(key_list[6], (H3,), 0.5, 3.0, (), jnp.float32),
        "weight_four": scatter_about(key_list[7], (H3, H4), H3 ** -0.5, 0.25),
        "bias_four": scatter_about(key_list[8], (H4,), 0.5, 3.0, (), jnp.float32),
        "weight_out": scatter_about(key_list[9], (H4, 1), 0.2, 1.0),
        "bias_out": jnp.clip(jax.random.uniform(key_list[10], (1,), jnp.float32, -1.5, 0.0), -1.5, 0.0),
        "bucket_index": draw_bucket_index(jax.random.fold_in(key_list[13], 71), 0),
        "labels": draw_labels(jax.random.fold_in(key_list[13], 71), 0),
    }


def layer_relu(inputs, weight, offset):
    return jax.nn.relu(jnp.dot(inputs, weight, preferred_element_type=jnp.float32) + offset).astype(jnp.bfloat16)


def bucket_reports(totals):
    positives = totals[:, 0]
    negatives = totals[:, 1]
    counts = jnp.maximum(positives + negatives, 1.0)
    return jnp.stack([positives / counts, totals[:, 2] / counts, totals[:, 3] / counts, totals[:, 4] / counts], axis=1)


def summarize(numerator, column_sums):
    pair_count = jnp.maximum(column_sums[:, 0] * column_sums[:, 1], 1.0)
    example_count = jnp.maximum(column_sums[:, 0] + column_sums[:, 1], 1.0)
    return jnp.stack([numerator / pair_count, column_sums[:, 3] / example_count,
                      column_sums[:, 2] / jnp.maximum(column_sums[:, 0], 1.0),
                      column_sums[:, 4] / example_count], axis=1)


def reference(interact, weight_one, bias_one, weight_two, bias_two, weight_three, bias_three,
              weight_four, bias_four, weight_out, bias_out, bucket_index, labels):
    def one_interval(inputs):
        features, buckets, targets = inputs
        hidden = layer_relu(features, weight_one, bias_one)
        hidden = layer_relu(hidden, weight_two, bias_two)
        hidden = layer_relu(hidden, weight_three, bias_three)
        hidden = layer_relu(hidden, weight_four, bias_four)
        logits = jnp.dot(hidden, weight_out, preferred_element_type=jnp.float32)[:, 0] + bias_out[0]
        observed = targets.astype(jnp.float32)
        predicted = jax.nn.sigmoid(logits)
        losses = jax.nn.softplus(logits) - observed * logits
        squared = (predicted - observed) ** 2
        values = jnp.stack([observed, 1.0 - observed, predicted, losses, squared], axis=1)
        return jax.ops.segment_sum(values, buckets, num_segments=NBUCK).T

    totals = lax.map(one_interval, (interact, bucket_index, labels))
    negatives = totals[:, 1]
    below_count = jnp.cumsum(negatives, axis=1) - negatives
    numerator = jnp.sum(totals[:, 0] * (below_count + 0.5 * negatives), axis=1)
    return bucket_reports(totals), summarize(numerator, jnp.sum(totals, axis=2))
```

```python
import jax
import jax.numpy as jnp
from jax import lax
from jax.experimental import pallas as pl
from jax.experimental.pallas import tpu as pltpu
from jax.sharding import PartitionSpec as P

NBUCK = 4096
RANGE = 512
LOW = 64
HIGH = RANGE // LOW
ALL = ("gx", "gy", "gz")
ROWS_PER_STEP = 1024
PAYLOAD = 4 * RANGE + 128


def mlp_body(x, w1, b1, w2, b2, w3, b3, w4, b4, wo, bo, out):
    intervals = x.shape[0]
    rows = intervals * x.shape[1]
    chains = 4
    flat = x[...].reshape(rows, x.shape[2])
    size = rows // chains
    hidden = [flat[c * size : (c + 1) * size] for c in range(chains)]
    for w, b in ((w1, b1), (w2, b2), (w3, b3), (w4, b4)):
        hidden = [
            jnp.maximum(
                jnp.dot(h, w[...], preferred_element_type=jnp.float32) + b[...], 0.0
            ).astype(jnp.bfloat16)
            for h in hidden
        ]
    last = jnp.concatenate(hidden, axis=0)
    logits = (
        lax.dot_general(
            wo[...], last, (((1,), (1,)), ((), ())), preferred_element_type=jnp.float32
        )
        + bo[0]
    )
    per = x.shape[1]
    for i in range(intervals):
        row = logits[0:1, i * per : (i + 1) * per]
        for a in range(out.shape[0]):
            for c in range(out.shape[2]):
                out[a, i, c] = row


def mlp_logits(x, w1, b1, w2, b2, w3, b3, w4, b4, wo, bo, copies):
    intervals, per, _ = x.shape
    step = ROWS_PER_STEP // per
    before, after = copies
    whole = lambda a: pl.BlockSpec(a.shape, lambda i: (0,) * a.ndim)
    biases = [b.reshape(1, -1) for b in (b1, b2, b3, b4)]
    out_row = jnp.broadcast_to(wo.reshape(1, -1), (16, wo.shape[0]))
    ops = []
    for w, b in zip((w1, w2, w3, w4), biases):
        ops += [w, b]
    ops.append(out_row)
    return pl.pallas_call(
        mlp_body,
        grid=(intervals // step,),
        in_specs=[pl.BlockSpec((step, per, x.shape[2]), lambda i: (i, 0, 0))]
        + [whole(a) for a in ops]
        + [pl.BlockSpec(memory_space=pltpu.SMEM)],
        out_specs=pl.BlockSpec((before, step, after, 1, per), lambda i: (0, i, 0, 0, 0)),
        out_shape=jax.ShapeDtypeStruct((before, intervals, after, 1, per), jnp.float32),
        compiler_params=pltpu.CompilerParams(
            dimension_semantics=("arbitrary",), vmem_limit_bytes=56 * 2**20
        ),
        name="mlp",
    )(x, *ops, bo)


def one_hot_rows(index_row, count):
    rows = lax.broadcasted_iota(jnp.int32, (count, index_row.shape[1]), 0)
    return jnp.where(rows == index_row, 1.0, 0.0).astype(jnp.bfloat16)


def nt_dot(a, b):
    return lax.dot_general(a, b, (((1,), (1,)), ((), ())), preferred_element_type=jnp.float32)


def count_body(block, tags, rate, inverse, numerator, acc):
    sources = tags.shape[0]
    per = tags.shape[2] // 2
    group = 8
    acc[...] = jnp.zeros_like(acc)

    def step(g, carry):
        left, right = [], []
        for k in range(group):
            row = tags[g * group + k]
            bucket, label = row[:, :per], row[:, per:]
            digit = lax.shift_right_logical(bucket, 7) + 32 * (1 - label)
            left.append(one_hot_rows(digit, 64))
            right.append(one_hot_rows(jnp.bitwise_and(bucket, 127), 128))
        acc[...] += nt_dot(jnp.concatenate(left, 1), jnp.concatenate(right, 1))
        return carry

    lax.fori_loop(0, sources // group, step, 0)
    pos, neg = acc[0:32], acc[32:64]
    lane = lax.broadcasted_iota(jnp.int32, neg.shape, 1)
    sub = lax.broadcasted_iota(jnp.int32, neg.shape, 0)
    run = neg
    for shift in (1, 2, 4, 8, 16, 32, 64):
        run = run + jnp.where(lane >= shift, pltpu.roll(run, shift, 1), 0.0)
    total = jnp.broadcast_to(jnp.sum(neg, axis=1, keepdims=True), neg.shape)
    above = total
    for shift in (1, 2, 4, 8, 16):
        above = above + jnp.where(sub >= shift, pltpu.roll(above, shift, 0), 0.0)
    below = run - neg + above - total
    pairs = jnp.sum(pos * (below + 0.5 * neg))
    positives, negatives = jnp.sum(pos), jnp.sum(neg)
    pick = lax.broadcasted_iota(jnp.int32, (1, 128), 1)
    numerator[...] = jnp.where(
        pick == 0,
        pairs / jnp.maximum(positives * negatives, 1.0),
        jnp.where(
            pick == 2,
            1.0 / jnp.maximum(positives, 1.0),
            1.0 / jnp.maximum(positives + negatives, 1.0),
        ),
    )
    first = block[0] * 4
    own_pos, own_neg = acc[pl.ds(first, 4)], acc[pl.ds(first + 32, 4)]
    count = jnp.maximum(own_pos + own_neg, 1.0)
    rate[...] = own_pos / count
    inverse[...] = 1.0 / count


def value_body(block, tags, logits, rate, inverse, numerator, out, parts, digits):
    sources = tags.shape[0]
    per = logits.shape[2]
    z = logits[:, 0, :]
    bucket = tags[:, 0, :per]
    y = tags[:, 0, per:].astype(jnp.float32)
    p = jax.nn.sigmoid(z)
    loss = jax.nn.softplus(z) - y * z
    sq = (p - y) ** 2
    sums = []
    for v, value in enumerate((p, loss, sq)):
        upper = value.astype(jnp.bfloat16).astype(jnp.float32)
        parts[2 * v] = upper
        parts[2 * v + 1] = value - upper
        sums.append(jnp.sum(value))
    digits[0] = lax.shift_right_arithmetic(bucket - block[0] * RANGE, 6)
    digits[1] = jnp.bitwise_and(bucket, LOW - 1)
    group = 8

    def step(g, acc):
        left, right = [], []
        for k in range(group):
            i = g * group + k
            high = digits[0, pl.ds(i, 1), :]
            match = lax.broadcasted_iota(jnp.int32, (HIGH, per), 0) == high
            left.append(
                jnp.concatenate(
                    [jnp.where(match, parts[v, pl.ds(i, 1), :], 0.0) for v in range(6)], 0
                ).astype(jnp.bfloat16)
            )
            right.append(one_hot_rows(digits[1, pl.ds(i, 1), :], LOW))
        return acc + nt_dot(jnp.concatenate(left, 1), jnp.concatenate(right, 1))

    acc = lax.fori_loop(0, sources // group, step, jnp.zeros((6 * HIGH, LOW), jnp.float32))
    rows = [rate[...]]
    for v in range(3):
        both = acc[2 * v * HIGH : (2 * v + 1) * HIGH] + acc[(2 * v + 1) * HIGH : (2 * v + 2) * HIGH]
        rows.append(
            jnp.concatenate(
                [
                    jnp.concatenate([both[2 * t : 2 * t + 1], both[2 * t + 1 : 2 * t + 2]], 1)
                    for t in range(HIGH // 2)
                ],
                0,
            )
            * inverse[...]
        )
    copies = out.shape[0]
    for t in range(HIGH // 2):
        for r in range(4):
            at = (t * 4 + r) * 128
            out[:, 0, at : at + 128] = jnp.broadcast_to(rows[r][t : t + 1], (copies, 128))
    pick = lax.broadcasted_iota(jnp.int32, (1, 128), 1)
    scale = numerator[...]
    last = jnp.where(
        pick == 0,
        scale,
        scale * jnp.where(pick == 1, sums[1], jnp.where(pick == 2, sums[0], sums[2])),
    )
    out[:, 0, 4 * RANGE :] = jnp.broadcast_to(last, (copies, 128))


def call_counts(block, tags):
    vmem = pl.BlockSpec(memory_space=pltpu.VMEM)
    return pl.pallas_call(
        count_body,
        in_specs=[pl.BlockSpec(memory_space=pltpu.SMEM), vmem],
        out_specs=[vmem] * 3,
        out_shape=[
            jax.ShapeDtypeStruct((4, 128), jnp.float32),
            jax.ShapeDtypeStruct((4, 128), jnp.float32),
            jax.ShapeDtypeStruct((1, 128), jnp.float32),
        ],
        scratch_shapes=[pltpu.VMEM((64, 128), jnp.float32)],
        name="counts",
    )(block, tags)


def call_values(block, tags, logits, rate, inverse, numerator, copies):
    vmem = pl.BlockSpec(memory_space=pltpu.VMEM)
    sources, _, per = logits.shape
    return pl.pallas_call(
        value_body,
        in_specs=[pl.BlockSpec(memory_space=pltpu.SMEM)] + [vmem] * 5,
        out_specs=vmem,
        out_shape=jax.ShapeDtypeStruct((copies, 1, PAYLOAD), jnp.float32),
        scratch_shapes=[
            pltpu.VMEM((6, sources, per), jnp.float32),
            pltpu.VMEM((2, sources, per), jnp.int32),
        ],
        name="values",
    )(block, tags, logits, rate, inverse, numerator)


def on_device(
    interact,
    weight_one,
    bias_one,
    weight_two,
    bias_two,
    weight_three,
    bias_three,
    weight_four,
    bias_four,
    weight_out,
    bias_out,
    bucket_index,
    labels,
):
    intervals, per, _ = interact.shape
    sizes = [lax.axis_size(a) for a in ALL]
    everyone = sizes[0] * sizes[1] * sizes[2]
    before, after = sizes[0], 2
    tags = jnp.concatenate([bucket_index, labels], axis=1)
    tags = jnp.broadcast_to(
        tags[None, :, None, None], (before, intervals, after, 1, 2 * per)
    ).reshape(everyone, 1, 2 * per)
    tags = lax.all_to_all(tags, ALL, 0, 0, tiled=True)
    block = (lax.axis_index("gx") * 2 + lax.axis_index("gz") % 2).reshape(1).astype(jnp.int32)
    logits = mlp_logits(
        interact,
        weight_one,
        bias_one,
        weight_two,
        bias_two,
        weight_three,
        bias_three,
        weight_four,
        bias_four,
        weight_out,
        bias_out,
        (before, after),
    ).reshape(everyone, 1, per)
    logits = lax.all_to_all(logits, ALL, 0, 0, tiled=True)
    rate, inverse, numerator = call_counts(block, tags)
    group = sizes[1] * sizes[2]
    payload = call_values(block, tags, logits, rate, inverse, numerator, group)
    payload = lax.all_to_all(payload, ("gy", "gz"), 0, 0, tiled=True)
    payload = payload.reshape(intervals, after, PAYLOAD)
    reports = payload[:, :, : 4 * RANGE].reshape(intervals, after, RANGE // 128, 4, 128)
    reports = reports.transpose(0, 3, 1, 2, 4).reshape(intervals, 4, after * RANGE)
    return reports, payload[:, 0, 4 * RANGE : 4 * RANGE + 4]


def solution(mesh):
    split = P(None, ALL)
    in_specs = (P(None, ALL, None),) + (P(),) * 10 + (split, split)
    out_specs = (P(None, None, "gx"), P())
    return jax.shard_map(
        on_device, mesh=mesh, in_specs=in_specs, out_specs=out_specs, check_vma=False
    )
```

```python
import jax
import jax.numpy as jnp
from jax import lax
from jax.experimental import pallas as pl
from jax.experimental.pallas import tpu as pltpu
from jax.sharding import PartitionSpec as P

RANGE = 512
LOW = 128
OWN = RANGE // LOW
HIGH = 4096 // LOW
ALL = ("gx", "gy", "gz")
REPORT = 4 * RANGE
PAYLOAD = REPORT + 128
BF16 = jnp.bfloat16
F32 = jnp.float32


def in_vmem(value):
    return pltpu.with_memory_space_constraint(value, pltpu.VMEM)


def nt_dot(a, b):
    return lax.dot_general(a, b, (((1,), (1,)), ((), ())), preferred_element_type=F32)


def mlp_body(steps, chains, sources, bo, out, held, sem):
    x, buckets, labels = held[:3]
    intervals, per, width = x.shape
    each = intervals // steps
    copies = [
        pltpu.make_async_copy(src, dst, sem.at[steps + k])
        for k, (src, dst) in enumerate(zip(sources[1:], held[1:]))
    ]
    tags, weights, last_weight = copies[:2], copies[2:-1], copies[-1]
    feeds = []
    for k in range(steps):
        part = pl.ds(k * each, each)
        feeds.append(pltpu.make_async_copy(sources[0].at[part], x.at[part], sem.at[k]))
    for copy in feeds[:1] + weights + [last_weight] + tags + feeds[1:]:
        copy.start()

    def run(k, waiting):
        if waiting:
            feeds[0].wait()
        flat = x[pl.ds(k * each, each)].reshape(each * per, width)
        size = each * per // chains
        hidden = [flat[c * size : (c + 1) * size] for c in range(chains)]
        for j in range(4):
            w, b = held[3 + 2 * j], held[4 + 2 * j]
            if waiting:
                weights[2 * j].wait()
                weights[2 * j + 1].wait()
            hidden = [
                jnp.maximum(jnp.dot(h, w[...], preferred_element_type=F32) + b[...], 0.0).astype(
                    BF16
                )
                for h in hidden
            ]
        if waiting:
            for copy in [last_weight] + tags:
                copy.wait()
        column = jnp.broadcast_to(held[-1][...], (16, held[-1].shape[1]))
        logits = nt_dot(column, jnp.concatenate(hidden, axis=0)) + bo[0]
        for i in range(each):
            at = k * each + i
            row = jnp.concatenate(
                [
                    buckets[pl.ds(at, 1), :].astype(F32),
                    labels[pl.ds(at, 1), :].astype(F32),
                    logits[0:1, i * per : (i + 1) * per],
                ],
                axis=1,
            )
            for a in range(out.shape[0]):
                for c in range(out.shape[2]):
                    out[a, at, c] = row

    run(0, True)
    for copy in feeds[1:]:
        copy.wait()

    def step(k, carry):
        run(k, False)
        return carry

    lax.fori_loop(1, steps, step, 0)


def examples_to_send(x, buckets, labels, weights, biases, wo, bo, copies):
    intervals, per, _ = x.shape
    steps, chains = 4, 4
    before, after = copies
    ops = [x, buckets, labels]
    for w, b in zip(weights, biases):
        ops += [w, b.reshape(1, -1)]
    ops.append(wo.T)
    count = len(ops)

    def body(*refs):
        mlp_body(
            steps,
            chains,
            refs[:count],
            refs[count],
            refs[count + 1],
            refs[count + 2 : -1],
            refs[-1],
        )

    return pl.pallas_call(
        body,
        in_specs=[pl.BlockSpec(memory_space=pltpu.HBM)] * count
        + [pl.BlockSpec(memory_space=pltpu.SMEM)],
        out_specs=pl.BlockSpec(memory_space=pltpu.VMEM),
        out_shape=pltpu.VMEM((before, intervals, after, 1, 3 * per), F32),
        scratch_shapes=[pltpu.VMEM(a.shape, a.dtype) for a in ops]
        + [pltpu.SemaphoreType.DMA((steps + count - 1,))],
        compiler_params=pltpu.CompilerParams(vmem_limit_bytes=40 * 2**20),
        name="mlp",
    )(*[pltpu.with_memory_space_constraint(a, pltpu.HBM) for a in ops], bo)


def one_hot_rows(row, iota):
    wide = jnp.broadcast_to(row, (16, row.shape[1])).astype(BF16)
    one, zero = jnp.ones((), BF16), jnp.zeros((), BF16)
    return jnp.concatenate(
        [jnp.where(iota[k : k + 16] == wide, one, zero) for k in range(0, iota.shape[0], 16)], 0
    )


def histogram_body(rec, out, vals, digits, acc):
    sources = rec.shape[0]
    per = rec.shape[2] // 3
    group = 32
    block = lax.axis_index("gx") * 2 + lax.axis_index("gz") % 2
    bucket = rec[:, 0, :per].astype(jnp.int32)
    y = rec[:, 0, per : 2 * per]
    z = rec[:, 0, 2 * per :]
    p = jax.nn.sigmoid(z)
    loss = jax.nn.softplus(z) - y * z
    sq = (p - y) ** 2
    sums = []
    for v, value in enumerate((p, loss, sq)):
        upper = value.astype(BF16).astype(F32)
        vals[:, 2 * v, :] = upper
        vals[:, 2 * v + 1, :] = value - upper
        sums.append(jnp.sum(value))
    vals[:, 6, :] = jnp.zeros_like(y)
    vals[:, 7, :] = jnp.zeros_like(y)
    high = lax.shift_right_logical(bucket, 7)
    digits[0] = (high + jnp.where(y > 0.5, 0, HIGH)).astype(F32)
    digits[1] = jnp.bitwise_and(bucket, LOW - 1).astype(F32)
    digits[2] = (high - block * OWN).astype(F32)
    iota_high = lax.broadcasted_iota(jnp.int32, (2 * HIGH, per), 0).astype(F32).astype(BF16)
    iota_low = lax.broadcasted_iota(jnp.int32, (LOW, per), 0).astype(F32).astype(BF16)

    def step(g, carry):
        left, right = [], []
        for k in range(group):
            i = g * group + k
            own = jnp.broadcast_to(digits[2, pl.ds(i, 1), :], (8, per))
            mine = jnp.concatenate(
                [jnp.where(own == float(h), vals[i], 0.0) for h in range(OWN)], 0
            ).astype(BF16)
            counts = one_hot_rows(digits[0, pl.ds(i, 1), :], iota_high)
            left.append(jnp.concatenate([counts, mine], 0))
            right.append(one_hot_rows(digits[1, pl.ds(i, 1), :], iota_low))
        return carry + nt_dot(jnp.concatenate(left, 1), jnp.concatenate(right, 1))

    total = jnp.zeros((2 * HIGH + 8 * OWN, LOW), F32)
    total = lax.fori_loop(0, sources // group, step, total)
    acc[...] = total
    pos, neg = total[:HIGH], total[HIGH : 2 * HIGH]
    lane = lax.broadcasted_iota(jnp.int32, neg.shape, 1)
    sub = lax.broadcasted_iota(jnp.int32, neg.shape, 0)
    run = neg
    for shift in (1, 2, 4, 8, 16, 32, 64):
        run = run + jnp.where(lane >= shift, pltpu.roll(run, shift, 1), 0.0)
    line = jnp.broadcast_to(jnp.sum(neg, axis=1, keepdims=True), neg.shape)
    above = line
    for shift in (1, 2, 4, 8, 16):
        above = above + jnp.where(sub >= shift, pltpu.roll(above, shift, 0), 0.0)
    below = run - neg + above - line
    pairs = jnp.sum(pos * (below + 0.5 * neg))
    positives, negatives = jnp.sum(pos), jnp.sum(neg)
    first = block * OWN
    own_pos, own_neg = acc[pl.ds(first, OWN)], acc[pl.ds(first + HIGH, OWN)]
    inverse = 1.0 / jnp.maximum(own_pos + own_neg, 1.0)
    copies = out.shape[0]
    for t in range(OWN):
        scale = inverse[t : t + 1]
        for r in range(4):
            at = 2 * HIGH + 8 * t + 2 * (r - 1)
            sum_row = total[at : at + 1] + total[at + 1 : at + 2] if r else own_pos[t : t + 1]
            to = (t * 4 + r) * LOW
            out[:, 0, to : to + LOW] = jnp.broadcast_to(sum_row * scale, (copies, LOW))
    pick = lax.broadcasted_iota(jnp.int32, (1, 128), 1)
    upper_part = jnp.where(
        pick == 0, pairs, jnp.where(pick == 1, sums[1], jnp.where(pick == 2, sums[0], sums[2]))
    )
    lower_part = jnp.where(
        pick == 0,
        positives * negatives,
        jnp.where(pick == 2, positives, positives + negatives),
    )
    last = upper_part / jnp.maximum(lower_part, 1.0)
    out[:, 0, REPORT:] = jnp.broadcast_to(last, (copies, 128))


def reports_to_send(rec, copies):
    vmem = pl.BlockSpec(memory_space=pltpu.VMEM)
    sources, _, three = rec.shape
    per = three // 3
    return pl.pallas_call(
        histogram_body,
        in_specs=[vmem],
        out_specs=vmem,
        out_shape=pltpu.VMEM((copies, 1, PAYLOAD), F32),
        scratch_shapes=[
            pltpu.VMEM((sources, 8, per), F32),
            pltpu.VMEM((3, sources, per), F32),
            pltpu.VMEM((2 * HIGH + 8 * OWN, LOW), F32),
        ],
        name="histogram",
    )(in_vmem(rec))


def arrange_body(rec, reports, summary):
    parts = rec.shape[1]
    for t in range(OWN):
        for r in range(4):
            at = (t * 4 + r) * LOW
            for c in range(parts):
                to = c * RANGE + t * LOW
                reports[:, r, to : to + LOW] = rec[:, c, 0, at : at + LOW]
    rows = rec[:, 0, 0, REPORT:]
    fill = jnp.zeros((128 - rows.shape[0], 128), F32)
    summary[...] = jnp.concatenate([rows, fill], 0).T[:4, : rows.shape[0]]


def arranged(rec, intervals):
    vmem = pl.BlockSpec(memory_space=pltpu.VMEM)
    parts = rec.shape[0] // intervals
    rec = rec.reshape(intervals, parts, 1, PAYLOAD)
    reports, summary = pl.pallas_call(
        arrange_body,
        in_specs=[vmem],
        out_specs=[vmem, vmem],
        out_shape=[
            jax.ShapeDtypeStruct((intervals, 4, parts * RANGE), F32),
            jax.ShapeDtypeStruct((4, intervals), F32),
        ],
        name="arrange",
    )(in_vmem(rec))
    return reports, summary.T


def on_device(
    interact,
    weight_one,
    bias_one,
    weight_two,
    bias_two,
    weight_three,
    bias_three,
    weight_four,
    bias_four,
    weight_out,
    bias_out,
    bucket_index,
    labels,
):
    intervals, per, _ = interact.shape
    size_x, size_y, size_z = [lax.axis_size(a) for a in ALL]
    examples = examples_to_send(
        interact,
        bucket_index,
        labels,
        (weight_one, weight_two, weight_three, weight_four),
        (bias_one, bias_two, bias_three, bias_four),
        weight_out,
        bias_out,
        (size_x, 2),
    ).reshape(size_x * size_y * size_z, 1, 3 * per)
    examples = lax.all_to_all(examples, ALL, 0, 0, tiled=True)
    payload = reports_to_send(examples, size_y * size_z)
    payload = lax.all_to_all(payload, ("gy", "gz"), 0, 0, tiled=True)
    return arranged(payload, intervals)


def solution(mesh):
    split = P(None, ALL)
    in_specs = (P(None, ALL, None),) + (P(),) * 10 + (split, split)
    out_specs = (P(None, None, "gx"), P())
    return jax.shard_map(
        on_device, mesh=mesh, in_specs=in_specs, out_specs=out_specs, check_vma=False
    )
```

```python
import jax
import jax.numpy as jnp
from jax import lax
from jax.experimental import pallas as pl
from jax.experimental.pallas import tpu as pltpu
from jax.sharding import PartitionSpec as P

RANGE = 512
LOW = 128
OWN = RANGE // LOW
HIGH = 4096 // LOW
ALL = ("gx", "gy", "gz")
REPORT = 4 * RANGE
PAYLOAD = REPORT + 128
BF16 = jnp.bfloat16
F32 = jnp.float32


def in_vmem(value):
    return pltpu.with_memory_space_constraint(value, pltpu.VMEM)


def nt_dot(a, b):
    return lax.dot_general(a, b, (((1,), (1,)), ((), ())), preferred_element_type=F32)


def mlp_body(steps, chains, sources, bo, out, held, sem):
    x, buckets, labels = held[:3]
    intervals, per, width = x.shape
    each = intervals // steps
    copies = [
        pltpu.make_async_copy(src, dst, sem.at[steps + k])
        for k, (src, dst) in enumerate(zip(sources[1:], held[1:]))
    ]
    tags, weights, last_weight = copies[:2], copies[2:-1], copies[-1]
    feeds = []
    for k in range(steps):
        part = pl.ds(k * each, each)
        feeds.append(pltpu.make_async_copy(sources[0].at[part], x.at[part], sem.at[k]))
    for copy in feeds[:1] + weights + [last_weight] + tags + feeds[1:]:
        copy.start()

    def run(k, waiting):
        if waiting:
            feeds[0].wait()
        flat = x[pl.ds(k * each, each)].reshape(each * per, width)
        size = each * per // chains
        hidden = [flat[c * size : (c + 1) * size] for c in range(chains)]
        for j in range(4):
            w, b = held[3 + 2 * j], held[4 + 2 * j]
            if waiting:
                weights[2 * j].wait()
                weights[2 * j + 1].wait()
            hidden = [
                jnp.maximum(jnp.dot(h, w[...], preferred_element_type=F32) + b[...], 0.0).astype(
                    BF16
                )
                for h in hidden
            ]
        if waiting:
            for copy in [last_weight] + tags:
                copy.wait()
        column = jnp.broadcast_to(held[-1][...], (16, held[-1].shape[1]))
        logits = nt_dot(column, jnp.concatenate(hidden, axis=0)) + bo[0]
        for i in range(each):
            at = k * each + i
            row = jnp.concatenate(
                [
                    buckets[pl.ds(at, 1), :].astype(F32),
                    labels[pl.ds(at, 1), :].astype(F32),
                    logits[0:1, i * per : (i + 1) * per],
                ],
                axis=1,
            )
            for a in range(out.shape[0]):
                for c in range(out.shape[2]):
                    out[a, at, c] = row

    run(0, True)
    for copy in feeds[1:]:
        copy.wait()

    def step(k, carry):
        run(k, False)
        return carry

    lax.fori_loop(1, steps, step, 0)


def examples_to_send(x, buckets, labels, weights, biases, wo, bo, copies):
    intervals, per, _ = x.shape
    steps, chains = 4, 4
    before, after = copies
    ops = [x, buckets, labels]
    for w, b in zip(weights, biases):
        ops += [w, b.reshape(1, -1)]
    ops.append(wo.T)
    count = len(ops)

    def body(*refs):
        mlp_body(
            steps,
            chains,
            refs[:count],
            refs[count],
            refs[count + 1],
            refs[count + 2 : -1],
            refs[-1],
        )

    return pl.pallas_call(
        body,
        in_specs=[pl.BlockSpec(memory_space=pltpu.HBM)] * count
        + [pl.BlockSpec(memory_space=pltpu.SMEM)],
        out_specs=pl.BlockSpec(memory_space=pltpu.VMEM),
        out_shape=pltpu.VMEM((before, intervals, after, 1, 3 * per), F32),
        scratch_shapes=[pltpu.VMEM(a.shape, a.dtype) for a in ops]
        + [pltpu.SemaphoreType.DMA((steps + count - 1,))],
        compiler_params=pltpu.CompilerParams(vmem_limit_bytes=40 * 2**20),
        name="mlp",
    )(*[pltpu.with_memory_space_constraint(a, pltpu.HBM) for a in ops], bo)


def one_hot_rows(row, iota):
    wide = jnp.broadcast_to(row, (16, row.shape[1])).astype(BF16)
    one, zero = jnp.ones((), BF16), jnp.zeros((), BF16)
    return jnp.concatenate(
        [jnp.where(iota[k : k + 16] == wide, one, zero) for k in range(0, iota.shape[0], 16)], 0
    )


def histogram_body(fields, rec, out, vals, digits, acc):
    stride = fields * 2
    sources = rec.shape[0] // stride
    chunks = 2 * sources
    group = 32
    block = lax.axis_index("gx") * 2 + lax.axis_index("gz") % 2
    sums = [0.0] * 3
    for half in range(2):
        bucket, y, z = [
            rec[pl.ds(2 * k + half, sources, stride=stride), :] for k in range(fields)
        ]
        bucket = bucket.astype(jnp.int32)
        p = jax.nn.sigmoid(z)
        loss = jax.nn.softplus(z) - y * z
        sq = (p - y) ** 2
        base = half * sources
        for v, value in enumerate((p, loss, sq)):
            upper = value.astype(BF16).astype(F32)
            vals[pl.ds(8 * base + 2 * v, sources, stride=8), :] = upper
            vals[pl.ds(8 * base + 2 * v + 1, sources, stride=8), :] = value - upper
            sums[v] += jnp.sum(value)
        for v in (6, 7):
            vals[pl.ds(8 * base + v, sources, stride=8), :] = jnp.zeros_like(y)
        high = lax.shift_right_logical(bucket, 7)
        part = pl.ds(base, sources)
        digits[0, part] = (high + jnp.where(y > 0.5, 0, HIGH)).astype(F32)
        digits[1, part] = jnp.bitwise_and(bucket, LOW - 1).astype(F32)
        digits[2, part] = (high - block * OWN).astype(F32)
    lanes = rec.shape[1]
    iota_high = lax.broadcasted_iota(jnp.int32, (2 * HIGH, lanes), 0).astype(F32).astype(BF16)
    iota_low = lax.broadcasted_iota(jnp.int32, (LOW, lanes), 0).astype(F32).astype(BF16)

    def step(g, carry):
        left, right = [], []
        for k in range(group):
            i = g * group + k
            own = jnp.broadcast_to(digits[2, pl.ds(i, 1), :], (8, lanes))
            value = vals[pl.ds(pl.multiple_of(8 * i, 8), 8), :]
            mine = jnp.concatenate(
                [jnp.where(own == float(h), value, 0.0) for h in range(OWN)], 0
            ).astype(BF16)
            counts = one_hot_rows(digits[0, pl.ds(i, 1), :], iota_high)
            left.append(jnp.concatenate([counts, mine], 0))
            right.append(one_hot_rows(digits[1, pl.ds(i, 1), :], iota_low))
        return carry + nt_dot(jnp.concatenate(left, 1), jnp.concatenate(right, 1))

    total = jnp.zeros((2 * HIGH + 8 * OWN, LOW), F32)
    total = lax.fori_loop(0, chunks // group, step, total)
    acc[...] = total
    pos, neg = total[:HIGH], total[HIGH : 2 * HIGH]
    lane = lax.broadcasted_iota(jnp.int32, neg.shape, 1)
    sub = lax.broadcasted_iota(jnp.int32, neg.shape, 0)
    run = neg
    for shift in (1, 2, 4, 8, 16, 32, 64):
        run = run + jnp.where(lane >= shift, pltpu.roll(run, shift, 1), 0.0)
    line = jnp.broadcast_to(jnp.sum(neg, axis=1, keepdims=True), neg.shape)
    above = line
    for shift in (1, 2, 4, 8, 16):
        above = above + jnp.where(sub >= shift, pltpu.roll(above, shift, 0), 0.0)
    below = run - neg + above - line
    pairs = jnp.sum(pos * (below + 0.5 * neg))
    positives, negatives = jnp.sum(pos), jnp.sum(neg)
    first = block * OWN
    own_pos, own_neg = acc[pl.ds(first, OWN)], acc[pl.ds(first + HIGH, OWN)]
    inverse = 1.0 / jnp.maximum(own_pos + own_neg, 1.0)
    rows_each = PAYLOAD // LOW
    copies = out.shape[0] // rows_each
    for t in range(OWN):
        scale = inverse[t : t + 1]
        for r in range(4):
            at = 2 * HIGH + 8 * t + 2 * (r - 1)
            sum_row = total[at : at + 1] + total[at + 1 : at + 2] if r else own_pos[t : t + 1]
            out[pl.ds(t * 4 + r, copies, stride=rows_each), :] = jnp.broadcast_to(
                sum_row * scale, (copies, LOW)
            )
    pick = lax.broadcasted_iota(jnp.int32, (1, LOW), 1)
    upper_part = jnp.where(
        pick == 0, pairs, jnp.where(pick == 1, sums[1], jnp.where(pick == 2, sums[0], sums[2]))
    )
    lower_part = jnp.where(
        pick == 0,
        positives * negatives,
        jnp.where(pick == 2, positives, positives + negatives),
    )
    last = upper_part / jnp.maximum(lower_part, 1.0)
    out[pl.ds(rows_each - 1, copies, stride=rows_each), :] = jnp.broadcast_to(last, (copies, LOW))


def reports_to_send(rec, copies):
    vmem = pl.BlockSpec(memory_space=pltpu.VMEM)
    fields = 3
    rec = rec.reshape(-1, LOW)
    chunks = rec.shape[0] // fields
    sent = pl.pallas_call(
        lambda *refs: histogram_body(fields, *refs),
        in_specs=[vmem],
        out_specs=vmem,
        out_shape=pltpu.VMEM((copies * PAYLOAD // LOW, LOW), F32),
        scratch_shapes=[
            pltpu.VMEM((8 * chunks, LOW), F32),
            pltpu.VMEM((3, chunks, LOW), F32),
            pltpu.VMEM((2 * HIGH + 8 * OWN, LOW), F32),
        ],
        name="histogram",
    )(in_vmem(rec))
    return sent.reshape(copies, 1, PAYLOAD)


def arrange_body(parts, rec, reports, summary):
    intervals = reports.shape[0]
    rows_each = PAYLOAD // LOW
    stride = parts * rows_each
    for t in range(OWN):
        for r in range(4):
            for c in range(parts):
                to = c * RANGE + t * LOW
                at = c * rows_each + t * 4 + r
                reports[:, r, to : to + LOW] = rec[pl.ds(at, intervals, stride=stride), :]
    rows = rec[pl.ds(rows_each - 1, intervals, stride=stride), :]
    fill = jnp.zeros((LOW - intervals, LOW), F32)
    summary[...] = jnp.concatenate([rows, fill], 0).T[:4, :intervals]


def arranged(rec, intervals):
    vmem = pl.BlockSpec(memory_space=pltpu.VMEM)
    parts = rec.shape[0] // intervals
    reports, summary = pl.pallas_call(
        lambda *refs: arrange_body(parts, *refs),
        in_specs=[vmem],
        out_specs=[vmem, vmem],
        out_shape=[
            jax.ShapeDtypeStruct((intervals, 4, parts * RANGE), F32),
            jax.ShapeDtypeStruct((4, intervals), F32),
        ],
        name="arrange",
    )(in_vmem(rec.reshape(-1, LOW)))
    return reports, summary.T


def on_device(
    interact,
    weight_one,
    bias_one,
    weight_two,
    bias_two,
    weight_three,
    bias_three,
    weight_four,
    bias_four,
    weight_out,
    bias_out,
    bucket_index,
    labels,
):
    intervals, per, _ = interact.shape
    size_x, size_y, size_z = [lax.axis_size(a) for a in ALL]
    examples = examples_to_send(
        interact,
        bucket_index,
        labels,
        (weight_one, weight_two, weight_three, weight_four),
        (bias_one, bias_two, bias_three, bias_four),
        weight_out,
        bias_out,
        (size_x, 2),
    ).reshape(size_x * size_y * size_z, 1, 3 * per)
    examples = lax.all_to_all(examples, ALL, 0, 0, tiled=True)
    payload = reports_to_send(examples, size_y * size_z)
    payload = lax.all_to_all(payload, ("gy", "gz"), 0, 0, tiled=True)
    return arranged(payload, intervals)


def solution(mesh):
    split = P(None, ALL)
    in_specs = (P(None, ALL, None),) + (P(),) * 10 + (split, split)
    out_specs = (P(None, None, "gx"), P())
    return jax.shard_map(
        on_device, mesh=mesh, in_specs=in_specs, out_specs=out_specs, check_vma=False
    )
```

```python
import jax
import jax.numpy as jnp
from jax import lax
from jax.experimental import pallas as pl
from jax.experimental.pallas import tpu as pltpu
from jax.sharding import PartitionSpec as P

RANGE = 512
LOW = 128
OWN = RANGE // LOW
HIGH = 4096 // LOW
ALL = ("gx", "gy", "gz")
REPORT = 4 * RANGE
PAYLOAD = REPORT + 128
BF16 = jnp.bfloat16
F32 = jnp.float32
POSITIVE = 4096.0


def in_vmem(value):
    return pltpu.with_memory_space_constraint(value, pltpu.VMEM)


def nt_dot(a, b):
    return lax.dot_general(a, b, (((1,), (1,)), ((), ())), preferred_element_type=F32)


def mlp_body(steps, chains, sources, bo, out, held, last, sem):
    x, buckets, labels = held[:3]
    intervals, per, width = x.shape
    each = intervals // steps
    copies = [
        pltpu.make_async_copy(src, dst, sem.at[steps + k])
        for k, (src, dst) in enumerate(zip(sources[1:], held[1:]))
    ]
    tags, weights, last_weight = copies[:2], copies[2:-1], copies[-1]
    feeds = []
    for k in range(steps):
        part = pl.ds(k * each, each)
        feeds.append(pltpu.make_async_copy(sources[0].at[part], x.at[part], sem.at[k]))
    for copy in feeds[:1] + weights + [last_weight] + tags + feeds[1:]:
        copy.start()

    def emit(k):
        column = held[-1][...].astype(F32)
        for i in range(each):
            at = k * each + i
            pieces = [buckets[pl.ds(at, 1), :].astype(F32), labels[pl.ds(at, 1), :].astype(F32)]
            for q in range(0, per, 128):
                h = last[pl.ds(i * per + q, 128), :].astype(F32) * column
                h = sum(h[:, j : j + 128] for j in range(0, h.shape[1], 128))
                pieces.append(jnp.sum(h.T, axis=0, keepdims=True) + bo[0])
            row = jnp.concatenate(pieces, axis=1)
            for a in range(out.shape[0]):
                for c in range(out.shape[2]):
                    out[a, at, c] = row

    def run(k, waiting):
        if waiting:
            feeds[0].wait()
        else:
            emit(k - 1)
        flat = x[pl.ds(k * each, each)].reshape(each * per, width)
        size = each * per // chains
        hidden = [flat[c * size : (c + 1) * size] for c in range(chains)]
        for j in range(4):
            w, b = held[3 + 2 * j], held[4 + 2 * j]
            if waiting:
                weights[2 * j].wait()
                weights[2 * j + 1].wait()
            hidden = [
                jnp.maximum(jnp.dot(h, w[...], preferred_element_type=F32) + b[...], 0.0).astype(
                    BF16
                )
                for h in hidden
            ]
        for c in range(chains):
            last[pl.ds(c * size, size), :] = hidden[c]

    run(0, True)
    for copy in [last_weight] + tags + feeds[1:]:
        copy.wait()

    def step(k, carry):
        run(k, False)
        return carry

    lax.fori_loop(1, steps, step, 0)
    emit(steps - 1)


def examples_to_send(x, buckets, labels, weights, biases, wo, bo, copies):
    intervals, per, _ = x.shape
    steps, chains = 4, 4
    before, after = copies
    ops = [x, buckets, labels]
    for w, b in zip(weights, biases):
        ops += [w, b.reshape(1, -1)]
    ops.append(wo.T)
    count = len(ops)

    def body(*refs):
        mlp_body(
            steps,
            chains,
            refs[:count],
            refs[count],
            refs[count + 1],
            refs[count + 2 : -2],
            refs[-2],
            refs[-1],
        )

    return pl.pallas_call(
        body,
        in_specs=[pl.BlockSpec(memory_space=pltpu.HBM)] * count
        + [pl.BlockSpec(memory_space=pltpu.SMEM)],
        out_specs=pl.BlockSpec(memory_space=pltpu.VMEM),
        out_shape=pltpu.VMEM((before, intervals, after, 1, 3 * per), F32),
        scratch_shapes=[pltpu.VMEM(a.shape, a.dtype) for a in ops]
        + [
            pltpu.VMEM((intervals // steps * per, wo.shape[0]), BF16),
            pltpu.SemaphoreType.DMA((steps + count - 1,)),
        ],
        compiler_params=pltpu.CompilerParams(vmem_limit_bytes=40 * 2**20),
        name="mlp",
    )(*[pltpu.with_memory_space_constraint(a, pltpu.HBM) for a in ops], bo)


def one_hot_rows(row, iota):
    wide = jnp.broadcast_to(row, (16, row.shape[1])).astype(BF16)
    one, zero = jnp.ones((), BF16), jnp.zeros((), BF16)
    return jnp.concatenate(
        [jnp.where(iota[k : k + 16] == wide, one, zero) for k in range(0, iota.shape[0], 16)], 0
    )


def histogram_body(fields, rec, out, vals, digits, acc):
    stride = fields * 2
    sources = rec.shape[0] // stride
    chunks = 2 * sources
    group = 16
    block = lax.axis_index("gx") * 2 + lax.axis_index("gz") % 2
    sums = [0.0] * 3
    for half in range(2):
        bucket, y, z = [
            rec[pl.ds(2 * k + half, sources, stride=stride), :] for k in range(fields)
        ]
        bucket = bucket.astype(jnp.int32)
        p = jax.nn.sigmoid(z)
        loss = jax.nn.softplus(z) - y * z
        sq = (p - y) ** 2
        base = half * sources
        for v, value in enumerate((p, loss, sq)):
            upper = value.astype(BF16).astype(F32)
            vals[pl.ds(8 * base + 2 * v, sources, stride=8), :] = upper
            vals[pl.ds(8 * base + 2 * v + 1, sources, stride=8), :] = value - upper
            sums[v] += jnp.sum(value)
        for v in (6, 7):
            vals[pl.ds(8 * base + v, sources, stride=8), :] = jnp.zeros_like(y)
        high = lax.shift_right_logical(bucket, 7)
        part = pl.ds(base, sources)
        digits[0, part] = high.astype(F32)
        digits[1, part] = jnp.bitwise_and(bucket, LOW - 1).astype(F32)
        digits[2, part] = jnp.where(y > 0.5, POSITIVE, 1.0)
    lanes = rec.shape[1]
    zero = jnp.zeros((), BF16)
    iota_high = lax.broadcasted_iota(jnp.int32, (HIGH, lanes), 0).astype(F32).astype(BF16)
    iota_low = lax.broadcasted_iota(jnp.int32, (LOW, lanes), 0).astype(F32).astype(BF16)
    pair = lax.broadcasted_iota(jnp.int32, (16, lanes), 0) // 8
    own_pairs = [(block * OWN + h + pair).astype(F32).astype(BF16) for h in range(0, OWN, 2)]

    def packed_row(k, i):
        return jnp.broadcast_to(digits[k, pl.ds(i, 1), :], (16, lanes)).astype(BF16)

    def hot(iota, digit, value):
        return [
            jnp.where(iota[k : k + 16] == digit, value, zero) for k in range(0, iota.shape[0], 16)
        ]

    def operands(i):
        digit, weight = packed_row(0, i), packed_row(2, i)
        value = vals[pl.ds(8 * i, 8), :]
        value = jnp.concatenate([value, value], 0).astype(BF16)
        left = hot(iota_high, digit, weight) + [jnp.where(m == digit, value, zero) for m in own_pairs]
        right = hot(iota_low, packed_row(1, i), jnp.ones((), BF16))
        return jnp.concatenate(left, 0), jnp.concatenate(right, 0)

    pos = neg = total = jnp.zeros((LOW, HIGH + 8 * OWN), F32)
    for g in range(chunks // group):
        ops = [operands(g * group + k) for k in range(group)]
        left = jnp.concatenate([o[0] for o in ops], 1)
        right = jnp.concatenate([o[1] for o in ops], 1)
        found = nt_dot(right, left)
        some = jnp.floor(found * (1.0 / POSITIVE))
        pos = pos + some
        neg = neg + (found - some * POSITIVE)
        total = total + found
    fill = jnp.zeros((LOW, 128 - 2 * HIGH - 8 * OWN), F32)
    wide = jnp.concatenate([pos[:, :HIGH], neg[:, :HIGH], total[:, HIGH:], fill], 1).T
    pos, neg = wide[:HIGH], wide[HIGH : 2 * HIGH]
    total = wide[2 * HIGH : 2 * HIGH + 8 * OWN]
    acc[:HIGH] = pos
    acc[HIGH:] = neg
    lane = lax.broadcasted_iota(jnp.int32, neg.shape, 1)
    sub = lax.broadcasted_iota(jnp.int32, neg.shape, 0)
    run = neg
    for shift in (1, 2, 4, 8, 16, 32, 64):
        run = run + jnp.where(lane >= shift, pltpu.roll(run, shift, 1), 0.0)
    line = jnp.broadcast_to(jnp.sum(neg, axis=1, keepdims=True), neg.shape)
    above = line
    for shift in (1, 2, 4, 8, 16):
        above = above + jnp.where(sub >= shift, pltpu.roll(above, shift, 0), 0.0)
    below = run - neg + above - line
    pairs = jnp.sum(pos * (below + 0.5 * neg))
    positives, negatives = jnp.sum(pos), jnp.sum(neg)
    first = block * OWN
    own_pos, own_neg = acc[pl.ds(first, OWN)], acc[pl.ds(first + HIGH, OWN)]
    inverse = 1.0 / jnp.maximum(own_pos + own_neg, 1.0)
    rows_each = PAYLOAD // LOW
    copies = out.shape[0] // rows_each
    for t in range(OWN):
        scale = inverse[t : t + 1]
        for r in range(4):
            at = 8 * t + 2 * (r - 1)
            sum_row = total[at : at + 1] + total[at + 1 : at + 2] if r else own_pos[t : t + 1]
            out[pl.ds(t * 4 + r, copies, stride=rows_each), :] = jnp.broadcast_to(
                sum_row * scale, (copies, LOW)
            )
    pick = lax.broadcasted_iota(jnp.int32, (1, LOW), 1)
    upper_part = jnp.where(
        pick == 0, pairs, jnp.where(pick == 1, sums[1], jnp.where(pick == 2, sums[0], sums[2]))
    )
    lower_part = jnp.where(
        pick == 0,
        positives * negatives,
        jnp.where(pick == 2, positives, positives + negatives),
    )
    last = upper_part / jnp.maximum(lower_part, 1.0)
    out[pl.ds(rows_each - 1, copies, stride=rows_each), :] = jnp.broadcast_to(last, (copies, LOW))


def reports_to_send(rec, copies):
    vmem = pl.BlockSpec(memory_space=pltpu.VMEM)
    fields = 3
    rec = rec.reshape(-1, LOW)
    chunks = rec.shape[0] // fields
    sent = pl.pallas_call(
        lambda *refs: histogram_body(fields, *refs),
        in_specs=[vmem],
        out_specs=vmem,
        out_shape=pltpu.VMEM((copies * PAYLOAD // LOW, LOW), F32),
        scratch_shapes=[
            pltpu.VMEM((8 * chunks, LOW), F32),
            pltpu.VMEM((3, chunks, LOW), F32),
            pltpu.VMEM((2 * HIGH, LOW), F32),
        ],
        name="histogram",
    )(in_vmem(rec))
    return sent.reshape(copies, 1, PAYLOAD)


def arrange_body(rec, reports, summary):
    intervals, parts = rec.shape[:2]
    for t in range(OWN):
        for r in range(4):
            at = (t * 4 + r) * LOW
            for c in range(parts):
                to = c * RANGE + t * LOW
                reports[:, r, to : to + LOW] = rec[:, c, 0, at : at + LOW]
    rows = rec[:, 0, 0, REPORT:]
    fill = jnp.zeros((128 - intervals, 128), F32)
    summary[...] = jnp.concatenate([rows, fill], 0).T[:4, :intervals]


def arranged(rec, intervals):
    vmem = pl.BlockSpec(memory_space=pltpu.VMEM)
    parts = rec.shape[0] // intervals
    rec = rec.reshape(intervals, parts, 1, PAYLOAD)
    reports, summary = pl.pallas_call(
        arrange_body,
        in_specs=[vmem],
        out_specs=[vmem, vmem],
        out_shape=[
            jax.ShapeDtypeStruct((intervals, 4, parts * RANGE), F32),
            jax.ShapeDtypeStruct((4, intervals), F32),
        ],
        name="arrange",
    )(in_vmem(rec))
    return reports, summary.T


def on_device(
    interact,
    weight_one,
    bias_one,
    weight_two,
    bias_two,
    weight_three,
    bias_three,
    weight_four,
    bias_four,
    weight_out,
    bias_out,
    bucket_index,
    labels,
):
    intervals, per, _ = interact.shape
    size_x, size_y, size_z = [lax.axis_size(a) for a in ALL]
    examples = examples_to_send(
        interact,
        bucket_index,
        labels,
        (weight_one, weight_two, weight_three, weight_four),
        (bias_one, bias_two, bias_three, bias_four),
        weight_out,
        bias_out,
        (size_x, 2),
    ).reshape(size_x * size_y * size_z, 1, 3 * per)
    examples = lax.all_to_all(examples, ALL, 0, 0, tiled=True)
    payload = reports_to_send(examples, size_y * size_z)
    payload = lax.all_to_all(payload, ("gy", "gz"), 0, 0, tiled=True)
    return arranged(payload, intervals)


def solution(mesh):
    split = P(None, ALL)
    in_specs = (P(None, ALL, None),) + (P(),) * 10 + (split, split)
    out_specs = (P(None, None, "gx"), P())
    return jax.shard_map(
        on_device, mesh=mesh, in_specs=in_specs, out_specs=out_specs, check_vma=False
    )
```

```python
import jax
import jax.numpy as jnp
from jax import lax
from jax.experimental import pallas as pl
from jax.experimental.pallas import tpu as pltpu
from jax.sharding import Mesh
from jax.sharding import PartitionSpec as P

RANGE = 512
LOW = 128
OWN = RANGE // LOW
HIGH = 4096 // LOW
ALL = ("gx", "gy", "gm", "core")
REPORT = 4 * RANGE
PAYLOAD = REPORT + 128
BF16 = jnp.bfloat16
F32 = jnp.float32
POSITIVE = 4096.0


def in_vmem(value):
    return pltpu.with_memory_space_constraint(value, pltpu.VMEM)


def nt_dot(a, b):
    return lax.dot_general(a, b, (((1,), (1,)), ((), ())), preferred_element_type=F32)


def mlp_body(steps, chains, sources, bo, out, held, last, sem):
    x, buckets, labels = held[:3]
    intervals, per, width = x.shape
    each = intervals // steps
    copies = [
        pltpu.make_async_copy(src, dst, sem.at[steps + k])
        for k, (src, dst) in enumerate(zip(sources[1:], held[1:]))
    ]
    tags, weights, last_weight = copies[:2], copies[2:-1], copies[-1]
    feeds = []
    for k in range(steps):
        part = pl.ds(k * each, each)
        feeds.append(pltpu.make_async_copy(sources[0].at[part], x.at[part], sem.at[k]))
    for copy in feeds[:1] + weights + [last_weight] + tags + feeds[1:]:
        copy.start()

    def emit(k):
        column = held[-1][...].astype(F32)
        for i in range(each):
            at = k * each + i
            pieces = [buckets[pl.ds(at, 1), :].astype(F32), labels[pl.ds(at, 1), :].astype(F32)]
            for q in range(0, per, 128):
                h = last[pl.ds(i * per + q, 128), :].astype(F32) * column
                h = sum(h[:, j : j + 128] for j in range(0, h.shape[1], 128))
                pieces.append(jnp.sum(h.T, axis=0, keepdims=True) + bo[0])
            row = jnp.concatenate(pieces, axis=1)
            for a in range(out.shape[0]):
                out[a, at] = row

    def run(k, waiting):
        if waiting:
            feeds[0].wait()
        else:
            emit(k - 1)
        flat = x[pl.ds(k * each, each)].reshape(each * per, width)
        size = each * per // chains
        hidden = [flat[c * size : (c + 1) * size] for c in range(chains)]
        for j in range(4):
            w, b = held[3 + 2 * j], held[4 + 2 * j]
            if waiting:
                weights[2 * j].wait()
                weights[2 * j + 1].wait()
            hidden = [
                jnp.maximum(jnp.dot(h, w[...], preferred_element_type=F32) + b[...], 0.0).astype(
                    BF16
                )
                for h in hidden
            ]
        for c in range(chains):
            last[pl.ds(c * size, size), :] = hidden[c]

    run(0, True)
    for copy in [last_weight] + tags + feeds[1:]:
        copy.wait()

    def step(k, carry):
        run(k, False)
        return carry

    lax.fori_loop(1, steps, step, 0)
    emit(steps - 1)


def examples_to_send(x, buckets, labels, weights, biases, wo, bo, copies):
    intervals, per, _ = x.shape
    steps, chains = 4, 4
    ops = [x, buckets, labels]
    for w, b in zip(weights, biases):
        ops += [w, b.reshape(1, -1)]
    ops.append(wo.T)
    count = len(ops)

    def body(*refs):
        mlp_body(
            steps,
            chains,
            refs[:count],
            refs[count],
            refs[count + 1],
            refs[count + 2 : -2],
            refs[-2],
            refs[-1],
        )

    return pl.pallas_call(
        body,
        in_specs=[pl.BlockSpec(memory_space=pltpu.HBM)] * count
        + [pl.BlockSpec(memory_space=pltpu.SMEM)],
        out_specs=pl.BlockSpec(memory_space=pltpu.VMEM),
        out_shape=pltpu.VMEM((copies, intervals, 1, 3 * per), F32),
        scratch_shapes=[pltpu.VMEM(a.shape, a.dtype) for a in ops]
        + [
            pltpu.VMEM((intervals // steps * per, wo.shape[0]), BF16),
            pltpu.SemaphoreType.DMA((steps + count - 1,)),
        ],
        compiler_params=pltpu.CompilerParams(vmem_limit_bytes=40 * 2**20),
        name="mlp",
    )(*[pltpu.with_memory_space_constraint(a, pltpu.HBM) for a in ops], bo)


def one_hot_rows(row, iota):
    wide = jnp.broadcast_to(row, (16, row.shape[1])).astype(BF16)
    one, zero = jnp.ones((), BF16), jnp.zeros((), BF16)
    return jnp.concatenate(
        [jnp.where(iota[k : k + 16] == wide, one, zero) for k in range(0, iota.shape[0], 16)], 0
    )


def own_block():
    return lax.axis_index("gx") * 2 + lax.axis_index("core")


def cell_sums(fields, rec, vals, digits):
    stride = fields * 2
    sources = rec.shape[0] // stride
    chunks = 2 * sources
    group = 16
    lanes = rec.shape[1]
    block = own_block()
    sums = [jnp.zeros((1, lanes), F32)] * 3
    for half in range(2):
        bucket, y, z = [
            rec[pl.ds(2 * k + half, sources, stride=stride), :] for k in range(fields)
        ]
        bucket = bucket.astype(jnp.int32)
        p = jax.nn.sigmoid(z)
        loss = jax.nn.softplus(z) - y * z
        sq = (p - y) ** 2
        base = half * sources
        for v, value in enumerate((p, loss, sq)):
            upper = value.astype(BF16).astype(F32)
            vals[pl.ds(8 * base + 2 * v, sources, stride=8), :] = upper
            vals[pl.ds(8 * base + 2 * v + 1, sources, stride=8), :] = value - upper
            sums[v] += jnp.sum(value, axis=0, keepdims=True)
        for v in (6, 7):
            vals[pl.ds(8 * base + v, sources, stride=8), :] = jnp.zeros_like(y)
        high = lax.shift_right_logical(bucket, 7)
        part = pl.ds(base, sources)
        digits[0, part] = high.astype(F32)
        digits[1, part] = jnp.bitwise_and(bucket, LOW - 1).astype(F32)
        digits[2, part] = jnp.where(y > 0.5, POSITIVE, 1.0)
    zero = jnp.zeros((), BF16)
    iota_high = lax.broadcasted_iota(jnp.int32, (HIGH, lanes), 0).astype(F32).astype(BF16)
    iota_low = lax.broadcasted_iota(jnp.int32, (LOW, lanes), 0).astype(F32).astype(BF16)
    pair = lax.broadcasted_iota(jnp.int32, (16, lanes), 0) // 8
    own_pairs = [(block * OWN + h + pair).astype(F32).astype(BF16) for h in range(0, OWN, 2)]

    def packed_row(k, i):
        return jnp.broadcast_to(digits[k, pl.ds(i, 1), :], (16, lanes)).astype(BF16)

    def hot(iota, digit, value):
        return [
            jnp.where(iota[k : k + 16] == digit, value, zero) for k in range(0, iota.shape[0], 16)
        ]

    def operands(i):
        digit, weight = packed_row(0, i), packed_row(2, i)
        value = vals[pl.ds(8 * i, 8), :]
        value = jnp.concatenate([value, value], 0).astype(BF16)
        left = hot(iota_high, digit, weight) + [jnp.where(m == digit, value, zero) for m in own_pairs]
        right = hot(iota_low, packed_row(1, i), jnp.ones((), BF16))
        return jnp.concatenate(left, 0), jnp.concatenate(right, 0)

    pos = neg = total = jnp.zeros((LOW, HIGH + 8 * OWN), F32)
    for g in range(chunks // group):
        ops = [operands(g * group + k) for k in range(group)]
        left = jnp.concatenate([o[0] for o in ops], 1)
        right = jnp.concatenate([o[1] for o in ops], 1)
        found = nt_dot(right, left)
        some = jnp.floor(found * (1.0 / POSITIVE))
        pos = pos + some
        neg = neg + (found - some * POSITIVE)
        total = total + found
    return (pos, neg, total), sums


def first_body(fields, rec, cells, sums, vals, digits):
    found, rows = cell_sums(fields, rec, vals, digits)
    for k in range(3):
        cells[k] = found[k]
        sums[k : k + 1] = rows[k]


def second_body(fields, rec, cells, sums_before, out, vals, digits, acc):
    found, rows = cell_sums(fields, rec, vals, digits)
    pos, neg, total = [found[k] + cells[k] for k in range(3)]
    sums = [jnp.sum(rows[k] + sums_before[k : k + 1]) for k in range(3)]
    block = own_block()
    fill = jnp.zeros((LOW, 128 - 2 * HIGH - 8 * OWN), F32)
    wide = jnp.concatenate([pos[:, :HIGH], neg[:, :HIGH], total[:, HIGH:], fill], 1).T
    pos, neg = wide[:HIGH], wide[HIGH : 2 * HIGH]
    total = wide[2 * HIGH : 2 * HIGH + 8 * OWN]
    acc[:HIGH] = pos
    acc[HIGH:] = neg
    lane = lax.broadcasted_iota(jnp.int32, neg.shape, 1)
    sub = lax.broadcasted_iota(jnp.int32, neg.shape, 0)
    run = neg
    for shift in (1, 2, 4, 8, 16, 32, 64):
        run = run + jnp.where(lane >= shift, pltpu.roll(run, shift, 1), 0.0)
    line = jnp.broadcast_to(jnp.sum(neg, axis=1, keepdims=True), neg.shape)
    above = line
    for shift in (1, 2, 4, 8, 16):
        above = above + jnp.where(sub >= shift, pltpu.roll(above, shift, 0), 0.0)
    below = run - neg + above - line
    pairs = jnp.sum(pos * (below + 0.5 * neg))
    positives, negatives = jnp.sum(pos), jnp.sum(neg)
    first = block * OWN
    own_pos, own_neg = acc[pl.ds(first, OWN)], acc[pl.ds(first + HIGH, OWN)]
    inverse = 1.0 / jnp.maximum(own_pos + own_neg, 1.0)
    rows_each = PAYLOAD // LOW
    copies = out.shape[0] // rows_each
    for t in range(OWN):
        scale = inverse[t : t + 1]
        for r in range(4):
            at = 8 * t + 2 * (r - 1)
            sum_row = total[at : at + 1] + total[at + 1 : at + 2] if r else own_pos[t : t + 1]
            out[pl.ds(t * 4 + r, copies, stride=rows_each), :] = jnp.broadcast_to(
                sum_row * scale, (copies, LOW)
            )
    pick = lax.broadcasted_iota(jnp.int32, (1, LOW), 1)
    upper_part = jnp.where(
        pick == 0, pairs, jnp.where(pick == 1, sums[1], jnp.where(pick == 2, sums[0], sums[2]))
    )
    lower_part = jnp.where(
        pick == 0,
        positives * negatives,
        jnp.where(pick == 2, positives, positives + negatives),
    )
    last = upper_part / jnp.maximum(lower_part, 1.0)
    out[pl.ds(rows_each - 1, copies, stride=rows_each), :] = jnp.broadcast_to(last, (copies, LOW))


def reports_to_send(rec, other, copies):
    vmem = pl.BlockSpec(memory_space=pltpu.VMEM)
    fields = 3
    rec, other = rec.reshape(-1, LOW), other.reshape(-1, LOW)
    chunks = rec.shape[0] // fields
    scratch = [pltpu.VMEM((8 * chunks, LOW), F32), pltpu.VMEM((3, chunks, LOW), F32)]
    cells, sums = pl.pallas_call(
        lambda *refs: first_body(fields, *refs),
        in_specs=[vmem],
        out_specs=[vmem, vmem],
        out_shape=[pltpu.VMEM((3, LOW, HIGH + 8 * OWN), F32), pltpu.VMEM((8, LOW), F32)],
        scratch_shapes=scratch,
        name="histogram_first",
    )(in_vmem(rec))
    sent = pl.pallas_call(
        lambda *refs: second_body(fields, *refs),
        in_specs=[vmem] * 3,
        out_specs=vmem,
        out_shape=pltpu.VMEM((copies * PAYLOAD // LOW, LOW), F32),
        scratch_shapes=scratch + [pltpu.VMEM((2 * HIGH, LOW), F32)],
        name="histogram_second",
    )(in_vmem(other), in_vmem(cells), in_vmem(sums))
    return sent.reshape(copies, 1, PAYLOAD)


def arrange_body(rec, reports, summary):
    intervals, parts = rec.shape[:2]
    for t in range(OWN):
        for r in range(4):
            at = (t * 4 + r) * LOW
            for c in range(parts):
                to = c * RANGE + t * LOW
                reports[:, r, to : to + LOW] = rec[:, c, 0, at : at + LOW]
    rows = rec[:, 0, 0, REPORT:]
    fill = jnp.zeros((128 - intervals, 128), F32)
    summary[...] = jnp.concatenate([rows, fill], 0).T[:4, :intervals]


def arranged(rec, intervals):
    vmem = pl.BlockSpec(memory_space=pltpu.VMEM)
    parts = rec.shape[0] // intervals
    rec = rec.reshape(intervals, parts, 1, PAYLOAD)
    reports, summary = pl.pallas_call(
        arrange_body,
        in_specs=[vmem],
        out_specs=[vmem, vmem],
        out_shape=[
            jax.ShapeDtypeStruct((intervals, 4, parts * RANGE), F32),
            jax.ShapeDtypeStruct((4, intervals), F32),
        ],
        name="arrange",
    )(in_vmem(rec))
    return reports, summary.T


def on_device(
    interact,
    weight_one,
    bias_one,
    weight_two,
    bias_two,
    weight_three,
    bias_three,
    weight_four,
    bias_four,
    weight_out,
    bias_out,
    bucket_index,
    labels,
):
    intervals, per, _ = interact.shape
    size_x, size_y, size_m, size_c = [lax.axis_size(a) for a in ALL]
    examples = examples_to_send(
        interact,
        bucket_index,
        labels,
        (weight_one, weight_two, weight_three, weight_four),
        (bias_one, bias_two, bias_three, bias_four),
        weight_out,
        bias_out,
        size_x,
    ).reshape(size_x * size_y * size_m, 1, 3 * per)
    examples = lax.all_to_all(examples, ALL[:3], 0, 0, tiled=True)
    others = lax.ppermute(examples, "core", [(0, 1), (1, 0)])
    payload = reports_to_send(examples, others, size_y * size_m * size_c)
    payload = lax.all_to_all(payload, ALL[1:], 0, 0, tiled=True)
    return arranged(payload, intervals)


def solution(mesh):
    x, y, z = [mesh.shape[a] for a in ("gx", "gy", "gz")]
    mesh = Mesh(mesh.devices.reshape(x, y, z // 2, 2), ALL)
    split = P(None, ALL)
    in_specs = (P(None, ALL, None),) + (P(),) * 10 + (split, split)
    out_specs = (P(None, None, "gx"), P())
    return jax.shard_map(
        on_device, mesh=mesh, in_specs=in_specs, out_specs=out_specs, check_vma=False
    )
```

```python
import jax
import jax.numpy as jnp
from jax import lax
from jax.experimental import pallas as pl
from jax.experimental.pallas import tpu as pltpu
from jax.sharding import Mesh
from jax.sharding import PartitionSpec as P

RANGE = 512
LOW = 128
OWN = RANGE // LOW
HIGH = 4096 // LOW
ALL = ("gx", "gy", "gm", "core")
REPORT = 4 * RANGE
PAYLOAD = REPORT + 128
BF16 = jnp.bfloat16
F32 = jnp.float32
POSITIVE = 4096.0


def in_vmem(value):
    return pltpu.with_memory_space_constraint(value, pltpu.VMEM)


def nt_dot(a, b):
    return lax.dot_general(a, b, (((1,), (1,)), ((), ())), preferred_element_type=F32)


def mlp_body(steps, chains, sources, bo, out, held, last, sem):
    x, buckets, labels = held[:3]
    intervals, per, width = x.shape
    each = intervals // steps
    copies = [
        pltpu.make_async_copy(src, dst, sem.at[steps + k])
        for k, (src, dst) in enumerate(zip(sources[1:], held[1:]))
    ]
    tags, weights, last_weight = copies[:2], copies[2:-1], copies[-1]
    feeds = []
    for k in range(steps):
        part = pl.ds(k * each, each)
        feeds.append(pltpu.make_async_copy(sources[0].at[part], x.at[part], sem.at[k]))
    for copy in feeds[:1] + weights + [last_weight] + tags + feeds[1:]:
        copy.start()

    def emit(k):
        column = held[-1][...].astype(F32)
        for i in range(each):
            at = k * each + i
            pieces = [buckets[pl.ds(at, 1), :].astype(F32), labels[pl.ds(at, 1), :].astype(F32)]
            for q in range(0, per, 128):
                h = last[pl.ds(i * per + q, 128), :].astype(F32) * column
                h = sum(h[:, j : j + 128] for j in range(0, h.shape[1], 128))
                pieces.append(jnp.sum(h.T, axis=0, keepdims=True) + bo[0])
            row = jnp.concatenate(pieces, axis=1)
            for a in range(out.shape[0]):
                out[a, at] = row

    layers = [(held[3 + 2 * j], held[4 + 2 * j]) for j in range(4)]
    size = each * per // chains
    for copy in feeds[:1] + weights[:2]:
        copy.wait()
    due = {0: weights[2:4], 1: weights[4:] + [last_weight] + tags + feeds[1:]}
    for k in range(steps):
        if k:
            emit(k - 1)
        flat = x[pl.ds(k * each, each)].reshape(each * per, width)
        hidden = [flat[c * size : (c + 1) * size] for c in range(chains)]
        for j, (w, b) in enumerate(layers):
            for c in range(chains):
                if k == 0 and c == chains - 1:
                    for copy in due.get(j, []):
                        copy.wait()
                found = jnp.dot(hidden[c], w[...], preferred_element_type=F32) + b[...]
                hidden[c] = jnp.maximum(found, 0.0).astype(BF16)
        for c in range(chains):
            last[pl.ds(c * size, size), :] = hidden[c]
    emit(steps - 1)


def examples_to_send(x, buckets, labels, weights, biases, wo, bo, copies):
    intervals, per, _ = x.shape
    steps, chains = 4, 4
    ops = [x, buckets, labels]
    for w, b in zip(weights, biases):
        ops += [w, b.reshape(1, -1)]
    ops.append(wo.T)
    count = len(ops)

    def body(*refs):
        mlp_body(
            steps,
            chains,
            refs[:count],
            refs[count],
            refs[count + 1],
            refs[count + 2 : -2],
            refs[-2],
            refs[-1],
        )

    return pl.pallas_call(
        body,
        in_specs=[pl.BlockSpec(memory_space=pltpu.HBM)] * count
        + [pl.BlockSpec(memory_space=pltpu.SMEM)],
        out_specs=pl.BlockSpec(memory_space=pltpu.VMEM),
        out_shape=pltpu.VMEM((copies, intervals, 1, 3 * per), F32),
        scratch_shapes=[pltpu.VMEM(a.shape, a.dtype) for a in ops]
        + [
            pltpu.VMEM((intervals // steps * per, wo.shape[0]), BF16),
            pltpu.SemaphoreType.DMA((steps + count - 1,)),
        ],
        compiler_params=pltpu.CompilerParams(
            vmem_limit_bytes=40 * 2**20
        ),
        name="mlp",
    )(*[pltpu.with_memory_space_constraint(a, pltpu.HBM) for a in ops], bo)


def one_hot_rows(row, iota):
    wide = jnp.broadcast_to(row, (16, row.shape[1])).astype(BF16)
    one, zero = jnp.ones((), BF16), jnp.zeros((), BF16)
    return jnp.concatenate(
        [jnp.where(iota[k : k + 16] == wide, one, zero) for k in range(0, iota.shape[0], 16)], 0
    )


def own_block():
    return lax.axis_index("gx") * 2 + lax.axis_index("core")


def cell_sums(fields, rec, vals, digits):
    stride = fields * 2
    sources = rec.shape[0] // stride
    chunks = 2 * sources
    group = 16
    lanes = rec.shape[1]
    block = own_block()
    sums = [jnp.zeros((1, lanes), F32)] * 3
    for half in range(2):
        bucket, y, z = [
            rec[pl.ds(2 * k + half, sources, stride=stride), :] for k in range(fields)
        ]
        bucket = bucket.astype(jnp.int32)
        p = jax.nn.sigmoid(z)
        loss = jax.nn.softplus(z) - y * z
        sq = (p - y) ** 2
        base = half * sources
        for v, value in enumerate((p, loss, sq)):
            upper = value.astype(BF16).astype(F32)
            vals[pl.ds(8 * base + 2 * v, sources, stride=8), :] = upper
            vals[pl.ds(8 * base + 2 * v + 1, sources, stride=8), :] = value - upper
            sums[v] += jnp.sum(value, axis=0, keepdims=True)
        for v in (6, 7):
            vals[pl.ds(8 * base + v, sources, stride=8), :] = jnp.zeros_like(y)
        high = lax.shift_right_logical(bucket, 7)
        part = pl.ds(base, sources)
        digits[0, part] = high.astype(F32)
        digits[1, part] = jnp.bitwise_and(bucket, LOW - 1).astype(F32)
        digits[2, part] = jnp.where(y > 0.5, POSITIVE, 1.0)
    zero = jnp.zeros((), BF16)
    iota_high = lax.broadcasted_iota(jnp.int32, (HIGH, lanes), 0).astype(F32).astype(BF16)
    iota_low = lax.broadcasted_iota(jnp.int32, (LOW, lanes), 0).astype(F32).astype(BF16)
    pair = lax.broadcasted_iota(jnp.int32, (16, lanes), 0) // 8
    own_pairs = [(block * OWN + h + pair).astype(F32).astype(BF16) for h in range(0, OWN, 2)]

    def packed_row(k, i):
        return jnp.broadcast_to(digits[k, pl.ds(i, 1), :], (16, lanes)).astype(BF16)

    def hot(iota, digit, value):
        return [
            jnp.where(iota[k : k + 16] == digit, value, zero) for k in range(0, iota.shape[0], 16)
        ]

    def operands(i):
        digit, weight = packed_row(0, i), packed_row(2, i)
        value = vals[pl.ds(8 * i, 8), :]
        value = jnp.concatenate([value, value], 0).astype(BF16)
        left = hot(iota_high, digit, weight) + [jnp.where(m == digit, value, zero) for m in own_pairs]
        right = hot(iota_low, packed_row(1, i), jnp.ones((), BF16))
        return jnp.concatenate(left, 0), jnp.concatenate(right, 0)

    pos = neg = total = jnp.zeros((LOW, HIGH + 8 * OWN), F32)
    for g in range(chunks // group):
        ops = [operands(g * group + k) for k in range(group)]
        left = jnp.concatenate([o[0] for o in ops], 1)
        right = jnp.concatenate([o[1] for o in ops], 1)
        found = nt_dot(right, left)
        some = jnp.floor(found * (1.0 / POSITIVE))
        pos = pos + some
        neg = neg + (found - some * POSITIVE)
        total = total + found
    return (pos, neg, total), sums


def first_body(fields, rec, cells, sums, vals, digits):
    found, rows = cell_sums(fields, rec, vals, digits)
    for k in range(3):
        cells[k] = found[k]
        sums[k : k + 1] = rows[k]


def second_body(fields, rec, cells, sums_before, out, vals, digits, acc):
    found, rows = cell_sums(fields, rec, vals, digits)
    pos, neg, total = [found[k] + cells[k] for k in range(3)]
    sums = [jnp.sum(rows[k] + sums_before[k : k + 1]) for k in range(3)]
    block = own_block()
    fill = jnp.zeros((LOW, 128 - 2 * HIGH - 8 * OWN), F32)
    wide = jnp.concatenate([pos[:, :HIGH], neg[:, :HIGH], total[:, HIGH:], fill], 1).T
    pos, neg = wide[:HIGH], wide[HIGH : 2 * HIGH]
    total = wide[2 * HIGH : 2 * HIGH + 8 * OWN]
    acc[:HIGH] = pos
    acc[HIGH:] = neg
    lane = lax.broadcasted_iota(jnp.int32, neg.shape, 1)
    sub = lax.broadcasted_iota(jnp.int32, neg.shape, 0)
    run = neg
    for shift in (1, 2, 4, 8, 16, 32, 64):
        run = run + jnp.where(lane >= shift, pltpu.roll(run, shift, 1), 0.0)
    line = jnp.broadcast_to(jnp.sum(neg, axis=1, keepdims=True), neg.shape)
    above = line
    for shift in (1, 2, 4, 8, 16):
        above = above + jnp.where(sub >= shift, pltpu.roll(above, shift, 0), 0.0)
    below = run - neg + above - line
    pairs = jnp.sum(pos * (below + 0.5 * neg))
    positives, negatives = jnp.sum(pos), jnp.sum(neg)
    first = block * OWN
    own_pos, own_neg = acc[pl.ds(first, OWN)], acc[pl.ds(first + HIGH, OWN)]
    inverse = 1.0 / jnp.maximum(own_pos + own_neg, 1.0)
    rows_each = PAYLOAD // LOW
    copies = out.shape[0] // rows_each
    for t in range(OWN):
        scale = inverse[t : t + 1]
        for r in range(4):
            at = 8 * t + 2 * (r - 1)
            sum_row = total[at : at + 1] + total[at + 1 : at + 2] if r else own_pos[t : t + 1]
            out[pl.ds(t * 4 + r, copies, stride=rows_each), :] = jnp.broadcast_to(
                sum_row * scale, (copies, LOW)
            )
    pick = lax.broadcasted_iota(jnp.int32, (1, LOW), 1)
    upper_part = jnp.where(
        pick == 0, pairs, jnp.where(pick == 1, sums[1], jnp.where(pick == 2, sums[0], sums[2]))
    )
    lower_part = jnp.where(
        pick == 0,
        positives * negatives,
        jnp.where(pick == 2, positives, positives + negatives),
    )
    last = upper_part / jnp.maximum(lower_part, 1.0)
    out[pl.ds(rows_each - 1, copies, stride=rows_each), :] = jnp.broadcast_to(last, (copies, LOW))


def reports_to_send(rec, other, copies):
    vmem = pl.BlockSpec(memory_space=pltpu.VMEM)
    fields = 3
    rec, other = rec.reshape(-1, LOW), other.reshape(-1, LOW)
    chunks = rec.shape[0] // fields
    scratch = [pltpu.VMEM((8 * chunks, LOW), F32), pltpu.VMEM((3, chunks, LOW), F32)]
    cells, sums = pl.pallas_call(
        lambda *refs: first_body(fields, *refs),
        in_specs=[vmem],
        out_specs=[vmem, vmem],
        out_shape=[pltpu.VMEM((3, LOW, HIGH + 8 * OWN), F32), pltpu.VMEM((8, LOW), F32)],
        scratch_shapes=scratch,
        name="histogram_first",
    )(in_vmem(rec))
    sent = pl.pallas_call(
        lambda *refs: second_body(fields, *refs),
        in_specs=[vmem] * 3,
        out_specs=vmem,
        out_shape=pltpu.VMEM((copies * PAYLOAD // LOW, LOW), F32),
        scratch_shapes=scratch + [pltpu.VMEM((2 * HIGH, LOW), F32)],
        name="histogram_second",
    )(in_vmem(other), in_vmem(cells), in_vmem(sums))
    return sent.reshape(copies, 1, PAYLOAD)


def arrange_body(rec, reports, summary):
    intervals, parts = rec.shape[:2]
    for t in range(OWN):
        for r in range(4):
            at = (t * 4 + r) * LOW
            for c in range(parts):
                to = c * RANGE + t * LOW
                reports[:, r, to : to + LOW] = rec[:, c, 0, at : at + LOW]
    rows = rec[:, 0, 0, REPORT:]
    fill = jnp.zeros((128 - intervals, 128), F32)
    summary[...] = jnp.concatenate([rows, fill], 0).T[:4, :intervals]


def arranged(rec, intervals):
    vmem = pl.BlockSpec(memory_space=pltpu.VMEM)
    parts = rec.shape[0] // intervals
    rec = rec.reshape(intervals, parts, 1, PAYLOAD)
    reports, summary = pl.pallas_call(
        arrange_body,
        in_specs=[vmem],
        out_specs=[vmem, vmem],
        out_shape=[
            jax.ShapeDtypeStruct((intervals, 4, parts * RANGE), F32),
            jax.ShapeDtypeStruct((4, intervals), F32),
        ],
        name="arrange",
    )(in_vmem(rec))
    return reports, summary.T


def on_device(
    interact,
    weight_one,
    bias_one,
    weight_two,
    bias_two,
    weight_three,
    bias_three,
    weight_four,
    bias_four,
    weight_out,
    bias_out,
    bucket_index,
    labels,
):
    intervals, per, _ = interact.shape
    size_x, size_y, size_m, size_c = [lax.axis_size(a) for a in ALL]
    examples = examples_to_send(
        interact,
        bucket_index,
        labels,
        (weight_one, weight_two, weight_three, weight_four),
        (bias_one, bias_two, bias_three, bias_four),
        weight_out,
        bias_out,
        size_x,
    ).reshape(size_x * size_y * size_m, 1, 3 * per)
    examples = lax.all_to_all(examples, ALL[:3], 0, 0, tiled=True)
    others = lax.ppermute(examples, "core", [(0, 1), (1, 0)])
    payload = reports_to_send(examples, others, size_y * size_m * size_c)
    payload = lax.all_to_all(payload, ALL[1:], 0, 0, tiled=True)
    return arranged(payload, intervals)


def solution(mesh):
    x, y, z = [mesh.shape[a] for a in ("gx", "gy", "gz")]
    mesh = Mesh(mesh.devices.reshape(x, y, z // 2, 2), ALL)
    split = P(None, ALL)
    in_specs = (P(None, ALL, None),) + (P(),) * 10 + (split, split)
    out_specs = (P(None, None, "gx"), P())
    return jax.shard_map(
        on_device, mesh=mesh, in_specs=in_specs, out_specs=out_specs, check_vma=False
    )
```

```python
import jax
import jax.numpy as jnp
from jax import lax
from jax.experimental import pallas as pl
from jax.experimental.pallas import tpu as pltpu
from jax.sharding import Mesh
from jax.sharding import PartitionSpec as P

RANGE = 512
LOW = 128
OWN = RANGE // LOW
HIGH = 4096 // LOW
ALL = ("gx", "gy", "gm", "core")
REPORT = 4 * RANGE
PAYLOAD = REPORT + 128
BF16 = jnp.bfloat16
F32 = jnp.float32
POSITIVE = 4096.0


def in_vmem(value):
    return pltpu.with_memory_space_constraint(value, pltpu.VMEM)


def nt_dot(a, b):
    return lax.dot_general(a, b, (((1,), (1,)), ((), ())), preferred_element_type=F32)


def mlp_body(steps, chains, sources, bo, out, held, last, sem):
    x, buckets, labels = held[:3]
    intervals, per, width = x.shape
    each = intervals // steps
    copies = [
        pltpu.make_async_copy(src, dst, sem.at[steps + k])
        for k, (src, dst) in enumerate(zip(sources[1:], held[1:]))
    ]
    tags, weights, last_weight = copies[:2], copies[2:-1], copies[-1]
    feeds = []
    for k in range(steps):
        part = pl.ds(k * each, each)
        feeds.append(pltpu.make_async_copy(sources[0].at[part], x.at[part], sem.at[k]))
    for copy in feeds[:1] + weights + [last_weight] + tags + feeds[1:]:
        copy.start()

    def emit(k):
        column = held[-1][...].astype(F32)
        for i in range(each):
            at = k * each + i
            pieces = [buckets[pl.ds(at, 1), :].astype(F32), labels[pl.ds(at, 1), :].astype(F32)]
            for q in range(0, per, 128):
                h = last[pl.ds(i * per + q, 128), :].astype(F32) * column
                h = sum(h[:, j : j + 128] for j in range(0, h.shape[1], 128))
                pieces.append(jnp.sum(h.T, axis=0, keepdims=True) + bo[0])
            row = jnp.concatenate(pieces, axis=1)
            for a in range(out.shape[0]):
                out[a, at] = row

    layers = [(held[3 + 2 * j], held[4 + 2 * j]) for j in range(4)]
    size = each * per // chains
    for copy in feeds[:1] + weights[:2]:
        copy.wait()
    due = {0: weights[2:4], 1: weights[4:] + [last_weight] + tags + feeds[1:]}
    for k in range(steps):
        if k:
            emit(k - 1)
        flat = x[pl.ds(k * each, each)].reshape(each * per, width)
        hidden = [flat[c * size : (c + 1) * size] for c in range(chains)]
        for j, (w, b) in enumerate(layers):
            for c in range(chains):
                if k == 0 and c == chains - 1:
                    for copy in due.get(j, []):
                        copy.wait()
                found = jnp.dot(hidden[c], w[...], preferred_element_type=F32) + b[...]
                hidden[c] = jnp.maximum(found, 0.0).astype(BF16)
        for c in range(chains):
            last[pl.ds(c * size, size), :] = hidden[c]
    emit(steps - 1)


def examples_to_send(x, buckets, labels, weights, biases, wo, bo, copies):
    intervals, per, _ = x.shape
    steps, chains = 4, 4
    ops = [x, buckets, labels]
    for w, b in zip(weights, biases):
        ops += [w, b.reshape(1, -1)]
    ops.append(wo.T)
    count = len(ops)

    def body(*refs):
        mlp_body(
            steps,
            chains,
            refs[:count],
            refs[count],
            refs[count + 1],
            refs[count + 2 : -2],
            refs[-2],
            refs[-1],
        )

    return pl.pallas_call(
        body,
        in_specs=[pl.BlockSpec(memory_space=pltpu.HBM)] * count
        + [pl.BlockSpec(memory_space=pltpu.SMEM)],
        out_specs=pl.BlockSpec(memory_space=pltpu.VMEM),
        out_shape=pltpu.VMEM((copies, intervals, 1, 3 * per), F32),
        scratch_shapes=[pltpu.VMEM(a.shape, a.dtype) for a in ops]
        + [
            pltpu.VMEM((intervals // steps * per, wo.shape[0]), BF16),
            pltpu.SemaphoreType.DMA((steps + count - 1,)),
        ],
        compiler_params=pltpu.CompilerParams(
            vmem_limit_bytes=40 * 2**20
        ),
        name="mlp",
    )(*[pltpu.with_memory_space_constraint(a, pltpu.HBM) for a in ops], bo)


def one_hot_rows(row, iota):
    wide = jnp.broadcast_to(row, (16, row.shape[1])).astype(BF16)
    one, zero = jnp.ones((), BF16), jnp.zeros((), BF16)
    return jnp.concatenate(
        [jnp.where(iota[k : k + 16] == wide, one, zero) for k in range(0, iota.shape[0], 16)], 0
    )


def own_block():
    return lax.axis_index("gx") * 2 + lax.axis_index("core")


def cell_sums(fields, rec, vals, digits):
    stride = fields * 2
    sources = rec.shape[0] // stride
    chunks = 2 * sources
    group = 16
    lanes = rec.shape[1]
    block = own_block()
    sums = [jnp.zeros((1, lanes), F32)] * 3
    for half in range(2):
        bucket, y, z = [
            rec[pl.ds(2 * k + half, sources, stride=stride), :] for k in range(fields)
        ]
        bucket = bucket.astype(jnp.int32)
        p = jax.nn.sigmoid(z)
        loss = jax.nn.softplus(z) - y * z
        sq = (p - y) ** 2
        base = half * sources
        for v, value in enumerate((p, loss, sq)):
            upper = value.astype(BF16).astype(F32)
            vals[pl.ds(8 * base + 2 * v, sources, stride=8), :] = upper
            vals[pl.ds(8 * base + 2 * v + 1, sources, stride=8), :] = value - upper
            sums[v] += jnp.sum(value, axis=0, keepdims=True)
        for v in (6, 7):
            vals[pl.ds(8 * base + v, sources, stride=8), :] = jnp.zeros_like(y)
        high = lax.shift_right_logical(bucket, 7)
        part = pl.ds(base, sources)
        digits[0, part] = high.astype(F32)
        digits[1, part] = jnp.bitwise_and(bucket, LOW - 1).astype(F32)
        digits[2, part] = jnp.where(y > 0.5, POSITIVE, 1.0)
    zero = jnp.zeros((), BF16)
    iota_high = lax.broadcasted_iota(jnp.int32, (HIGH, lanes), 0).astype(F32).astype(BF16)
    iota_low = lax.broadcasted_iota(jnp.int32, (LOW, lanes), 0).astype(F32).astype(BF16)
    pair = lax.broadcasted_iota(jnp.int32, (16, lanes), 0) // 8
    own_pairs = [(block * OWN + h + pair).astype(F32).astype(BF16) for h in range(0, OWN, 2)]

    def packed_row(k, i):
        return jnp.broadcast_to(digits[k, pl.ds(i, 1), :], (16, lanes)).astype(BF16)

    def hot(iota, digit, value):
        return [
            jnp.where(iota[k : k + 16] == digit, value, zero) for k in range(0, iota.shape[0], 16)
        ]

    def operands(i):
        digit, weight = packed_row(0, i), packed_row(2, i)
        value = vals[pl.ds(8 * i, 8), :]
        value = jnp.concatenate([value, value], 0).astype(BF16)
        left = hot(iota_high, digit, weight) + [jnp.where(m == digit, value, zero) for m in own_pairs]
        right = hot(iota_low, packed_row(1, i), jnp.ones((), BF16))
        return jnp.concatenate(left, 0), jnp.concatenate(right, 0)

    pos = neg = total = jnp.zeros((LOW, HIGH + 8 * OWN), F32)
    for g in range(chunks // group):
        ops = [operands(g * group + k) for k in range(group)]
        left = jnp.concatenate([o[0] for o in ops], 1)
        right = jnp.concatenate([o[1] for o in ops], 1)
        found = nt_dot(right, left)
        some = jnp.floor(found * (1.0 / POSITIVE))
        pos = pos + some
        neg = neg + (found - some * POSITIVE)
        total = total + found
    return (pos, neg, total), sums


def first_body(fields, rec, cells, sums, vals, digits):
    found, rows = cell_sums(fields, rec, vals, digits)
    for k in range(3):
        cells[k] = found[k]
        sums[k : k + 1] = rows[k]


def second_body(fields, rec, cells, sums_before, out, vals, digits, acc):
    found, rows = cell_sums(fields, rec, vals, digits)
    pos, neg, total = [found[k] + cells[k] for k in range(3)]
    sums = [jnp.sum(rows[k] + sums_before[k : k + 1]) for k in range(3)]
    block = own_block()
    fill = jnp.zeros((LOW, 128 - 2 * HIGH - 8 * OWN), F32)
    wide = jnp.concatenate([pos[:, :HIGH], neg[:, :HIGH], total[:, HIGH:], fill], 1).T
    pos, neg = wide[:HIGH], wide[HIGH : 2 * HIGH]
    total = wide[2 * HIGH : 2 * HIGH + 8 * OWN]
    acc[:HIGH] = pos
    acc[HIGH:] = neg
    neg_upper = jnp.floor(neg * (1.0 / 256.0))
    parts = [neg_upper.astype(BF16), (neg - neg_upper * 256.0).astype(BF16)]
    row, col = [lax.broadcasted_iota(jnp.int32, (LOW, LOW), d) for d in range(2)]
    earlier = jnp.where(row < col, 1.0, 0.0).astype(BF16)
    upto, of = [lax.broadcasted_iota(jnp.int32, (HIGH, HIGH), d) for d in range(2)]
    lower = jnp.where(of < upto, 1.0, 0.0).astype(BF16)
    dot = lambda a, b: jnp.dot(a, b, preferred_element_type=F32)
    within = dot(jnp.concatenate(parts, 0), earlier)
    within = within[:HIGH] * 256.0 + within[HIGH:]
    above = dot(lower, parts[0]) * 256.0 + dot(lower, parts[1])
    above = jnp.sum(above, axis=1, keepdims=True)
    pairs = jnp.sum(pos * (within + above + 0.5 * neg))
    positives, negatives = jnp.sum(pos), jnp.sum(neg)
    first = block * OWN
    own_pos, own_neg = acc[pl.ds(first, OWN)], acc[pl.ds(first + HIGH, OWN)]
    inverse = 1.0 / jnp.maximum(own_pos + own_neg, 1.0)
    rows_each = PAYLOAD // LOW
    copies = out.shape[0] // rows_each
    for t in range(OWN):
        scale = inverse[t : t + 1]
        for r in range(4):
            at = 8 * t + 2 * (r - 1)
            sum_row = total[at : at + 1] + total[at + 1 : at + 2] if r else own_pos[t : t + 1]
            out[pl.ds(t * 4 + r, copies, stride=rows_each), :] = jnp.broadcast_to(
                sum_row * scale, (copies, LOW)
            )
    pick = lax.broadcasted_iota(jnp.int32, (1, LOW), 1)
    upper_part = jnp.where(
        pick == 0, pairs, jnp.where(pick == 1, sums[1], jnp.where(pick == 2, sums[0], sums[2]))
    )
    lower_part = jnp.where(
        pick == 0,
        positives * negatives,
        jnp.where(pick == 2, positives, positives + negatives),
    )
    last = upper_part / jnp.maximum(lower_part, 1.0)
    out[pl.ds(rows_each - 1, copies, stride=rows_each), :] = jnp.broadcast_to(last, (copies, LOW))


def reports_to_send(rec, other, copies):
    vmem = pl.BlockSpec(memory_space=pltpu.VMEM)
    fields = 3
    rec, other = rec.reshape(-1, LOW), other.reshape(-1, LOW)
    chunks = rec.shape[0] // fields
    scratch = [pltpu.VMEM((8 * chunks, LOW), F32), pltpu.VMEM((3, chunks, LOW), F32)]
    cells, sums = pl.pallas_call(
        lambda *refs: first_body(fields, *refs),
        in_specs=[vmem],
        out_specs=[vmem, vmem],
        out_shape=[pltpu.VMEM((3, LOW, HIGH + 8 * OWN), F32), pltpu.VMEM((8, LOW), F32)],
        scratch_shapes=scratch,
        name="histogram_first",
    )(in_vmem(rec))
    sent = pl.pallas_call(
        lambda *refs: second_body(fields, *refs),
        in_specs=[vmem] * 3,
        out_specs=vmem,
        out_shape=pltpu.VMEM((copies * PAYLOAD // LOW, LOW), F32),
        scratch_shapes=scratch + [pltpu.VMEM((2 * HIGH, LOW), F32)],
        name="histogram_second",
    )(in_vmem(other), in_vmem(cells), in_vmem(sums))
    return sent.reshape(copies, 1, PAYLOAD)


def arrange_body(rec, reports, summary):
    intervals, parts = rec.shape[:2]
    for t in range(OWN):
        for r in range(4):
            at = (t * 4 + r) * LOW
            for c in range(parts):
                to = c * RANGE + t * LOW
                reports[:, r, to : to + LOW] = rec[:, c, 0, at : at + LOW]
    rows = rec[:, 0, 0, REPORT:]
    fill = jnp.zeros((128 - intervals, 128), F32)
    summary[...] = jnp.concatenate([rows, fill], 0).T[:4, :intervals]


def arranged(rec, intervals):
    vmem = pl.BlockSpec(memory_space=pltpu.VMEM)
    parts = rec.shape[0] // intervals
    rec = rec.reshape(intervals, parts, 1, PAYLOAD)
    reports, summary = pl.pallas_call(
        arrange_body,
        in_specs=[vmem],
        out_specs=[vmem, vmem],
        out_shape=[
            jax.ShapeDtypeStruct((intervals, 4, parts * RANGE), F32),
            jax.ShapeDtypeStruct((4, intervals), F32),
        ],
        name="arrange",
    )(in_vmem(rec))
    return reports, summary.T


def on_device(
    interact,
    weight_one,
    bias_one,
    weight_two,
    bias_two,
    weight_three,
    bias_three,
    weight_four,
    bias_four,
    weight_out,
    bias_out,
    bucket_index,
    labels,
):
    intervals, per, _ = interact.shape
    size_x, size_y, size_m, size_c = [lax.axis_size(a) for a in ALL]
    examples = examples_to_send(
        interact,
        bucket_index,
        labels,
        (weight_one, weight_two, weight_three, weight_four),
        (bias_one, bias_two, bias_three, bias_four),
        weight_out,
        bias_out,
        size_x,
    ).reshape(size_x * size_y * size_m, 1, 3 * per)
    examples = lax.all_to_all(examples, ALL[:3], 0, 0, tiled=True)
    others = lax.ppermute(examples, "core", [(0, 1), (1, 0)])
    payload = reports_to_send(examples, others, size_y * size_m * size_c)
    payload = lax.all_to_all(payload, ALL[1:], 0, 0, tiled=True)
    return arranged(payload, intervals)


def solution(mesh):
    x, y, z = [mesh.shape[a] for a in ("gx", "gy", "gz")]
    mesh = Mesh(mesh.devices.reshape(x, y, z // 2, 2), ALL)
    split = P(None, ALL)
    in_specs = (P(None, ALL, None),) + (P(),) * 10 + (split, split)
    out_specs = (P(None, None, "gx"), P())
    return jax.shard_map(
        on_device, mesh=mesh, in_specs=in_specs, out_specs=out_specs, check_vma=False
    )
```
